512 devices in a mesh: dp: 4 (over x), ep: 128 (over y, z, core).
Axes of the slice: x: 4, y: 8, z: 8, core: 2. Of those that a mesh axis runs over, the one named last changes fastest.
Arguments:
- tokens: bfloat16 [4096, 1024], P(('dp', 'ep')), may hold values from -6 to 6
- expert_ids: int32 [4096, 8], P(('dp', 'ep')), may hold values from 0 to 127, all different within a row; in each aligned block of 8 rows (0 to 7, 8 to 15, ...) no two rows name the same one
- gate_quant: int32 [4096, 8], P(('dp', 'ep')), may hold values from 1 to 1024
- bucket_ids: int32 [4096], P(('dp', 'ep')), may hold values from 0 to 15
- bucket_counts: int32 [16], replicated, may hold values from 0 to 512
- gate_weight: bfloat16 [128, 1024, 384], P('ep', 'dp'), may hold values from -0.1875 to 0.1875
- up_weight: bfloat16 [128, 1024, 384], P('ep', 'dp'), may hold values from -0.1875 to 0.1875
- down_weight: bfloat16 [128, 384, 1024], P('ep', 'dp'), may hold values from -0.3125 to 0.3125
- cotangent: bfloat16 [4096, 1024], P(('dp', 'ep')), may hold values from -6 to 6
Outputs:
- layer_out: bfloat16 [4096, 1024], P(('dp', 'ep'))
- token_grad: bfloat16 [4096, 1024], P(('dp', 'ep'))
- gate_grad: float32 [128, 1024, 384], P('ep', 'dp')
- up_grad: float32 [128, 1024, 384], P('ep', 'dp')
- down_grad: float32 [128, 384, 1024], P('ep', 'dp')
The draws below stay inside these ranges and needn't reach their ends.
Inputs may be any that keep to these rules, and one draw needn't show every extreme that they name: `expert_ids`: each row names 8 different experts. Among the 8 rows of one device no expert is named by more than 1 row, and in every draw some expert is named by exactly 1 row of some device.
All inputs are finite; a program needn't handle non-finite values.
Results may differ from the reference program's by a relative error of at most 0.0085.
Values may be sent and summed in bfloat16 or wider, within the bound.
A program may use at most 64 MiB of HBM per device.

```python
import math
import jax
import jax.numpy as jnp
import numpy as np
from jax import lax

D = 1024
FF = 384
TOP = 8
BUCKETS = 16
TOK_DEV = 8
EXPERTS = 128
CAP = 1
TOKENS = 4096
N_DP = 4
N_EP = 128


def touch_ends(values, rng, smallest, largest):
    place = [jax.random.randint(jax.random.fold_in(rng, axis), (), 0, length) for axis, length in enumerate(values.shape)]
    longest = values.shape.index(max(values.shape))
    next_to = place[:longest] + [(place[longest] + 1) % values.shape[longest]] + place[longest + 1:]
    return values.at[tuple(place)].set(smallest).at[tuple(next_to)].set(largest)


def level_of(key, dims, shards, least, largest):
    gain, own = 1.0, jax.random.fold_in(key, 6)
    for dim, parts in shards:
        heights = jnp.exp(jax.random.uniform(jax.random.fold_in(own, dim), (parts,), jnp.float32, least / len(shards), largest / len(shards)))
        gain = gain * jnp.repeat(heights, dims[dim] // parts).reshape([-1 if axis == dim else 1 for axis in range(len(dims))])
    return gain


def assign_block(own_key, own, number, rows, number_of, top, bound, skew):
    sequence = jax.random.permutation(own_key, number_of)
    heavy_load, ordinary = shares(number_of, rows * top, bound, skew, True), shares(number_of, rows * top, bound, skew, False)
    places = jnp.arange(number_of)

    def named(sizes, turn):
        used = int((sizes > 0).sum())
        fixed = max(1, used // 4)
        shifted = fixed + (places - fixed + turn * (used - fixed)) % max(1, number_of - fixed)
        return jnp.zeros((number_of,), jnp.int32).at[sequence[jnp.where(places < fixed, places, shifted)]].set(jnp.asarray(sizes, jnp.int32))

    sizes = jnp.where(number % 4 == 0, named(heavy_load, number // 4), named(ordinary, number - number // 4 - 1))
    mixed = jax.random.permutation(jax.random.fold_in(own, 3), number_of)
    donor, sink = mixed[0:number_of // 2 * 2:2], mixed[1:number_of // 2 * 2:2]
    room = jnp.minimum(sizes[donor] - 1, bound - sizes[sink]) // 2
    room = jnp.where((donor == sequence[0]) | (sink == sequence[0]) | (sizes[sink] == 0), 0, jnp.maximum(room, 0))
    shifted = jax.random.randint(jax.random.fold_in(own, 4), (number_of // 2,), 0, 1 << 20) % (room + 1)
    sizes = sizes.at[donor].add(-shifted).at[sink].add(shifted)
    items = jnp.searchsorted(jnp.cumsum(sizes), jnp.arange(rows * top), side="right").astype(jnp.int32)
    table = items.reshape(top, rows).T
    table = table[jax.random.permutation(jax.random.fold_in(own, 1), rows)]
    turn = jax.random.randint(jax.random.fold_in(own, 2), (rows, 1), 0, top)
    return jnp.take_along_axis(table, (jnp.arange(top)[None, :] + turn) % top, axis=1)


def shares(amount, total, bound, lean, full):
    weights = [(1 << 20) // math.isqrt(grade ** lean) + 1 for grade in range(1, amount + 1)]
    largest = bound if full else min(bound, max(-(-total // amount), total * weights[0] // sum(weights)))
    least = 1 if total - largest >= amount - 1 else 0
    counts, rest = [largest] + [least] * (amount - 1), total - largest - least * (amount - 1)
    while rest > 0:
        candidates = [i for i in range(1, amount) if counts[i] < largest] or [i for i in range(1, amount) if counts[i] < bound]
        whole, budget = sum([weights[i] for i in candidates]), rest
        for i in candidates:
            more = min(bound - counts[i], max(1, budget * weights[i] // whole), rest)
            counts[i] = counts[i] + more
            rest = rest - more
    return np.array(counts)


def gaussian(key, dims, width, bound, split=(), kind=jnp.bfloat16):
    loudness = level_of(key, dims, split, -0.22, 0.18) if split else 1.0
    entries = jax.random.normal(key, dims, jnp.float32) * width * loudness
    return jnp.minimum(jnp.maximum(entries, -bound), bound).astype(kind)


def setup_inputs(seed: int = 0) -> dict:
    key_of = jax.random.split(jax.random.key(seed), 10)
    tokens = gaussian(key_of[0], (TOKENS, D), 1.0, 6.0, ((0, 512),))
    expert_ids_keys = jax.random.split(jax.random.fold_in(key_of[1], 1), TOKENS // TOK_DEV)
    expert_ids_turns = jax.random.permutation(jax.random.fold_in(key_of[1], 3), TOKENS // TOK_DEV)
    expert_ids = jax.vmap(lambda own, number: assign_block(jax.random.fold_in(key_of[1], 2), own, number, TOK_DEV, EXPERTS, TOP, CAP, 2))(expert_ids_keys, expert_ids_turns).reshape((TOKENS, TOP))
    gate_quant = touch_ends(jax.random.randint(key_of[2], (TOKENS, TOP), 1, 1025), jax.random.fold_in(key_of[2], 1), 1, 1024).astype(jnp.int32)
    bucket_ids = touch_ends(jax.random.randint(key_of[3], (TOKENS,), 0, BUCKETS), jax.random.fold_in(key_of[3], 1), 0, BUCKETS - 1).astype(jnp.int32)
    bucket_counts = touch_ends(jax.random.randint(key_of[4], (BUCKETS,), 0, 513), jax.random.fold_in(key_of[4], 1), 0, 512).astype(jnp.int32)
    gate_weight = gaussian(key_of[5], (EXPERTS, D, FF), D ** -0.5, 0.1875, ((0, 128), (1, 4)))
    up_weight = gaussian(key_of[6], (EXPERTS, D, FF), D ** -0.5, 0.1875, ((0, 128), (1, 4)))
    down_weight = gaussian(key_of[7], (EXPERTS, FF, D), FF ** -0.5, 0.3125, ((0, 128), (1, 4)))
    cotangent = gaussian(key_of[8], (TOKENS, D), 1.0, 6.0, ((0, 512),))
    return {"tokens": tokens, "expert_ids": expert_ids, "gate_quant": gate_quant, "bucket_ids": bucket_ids, "bucket_counts": bucket_counts, "gate_weight": gate_weight, "up_weight": up_weight, "down_weight": down_weight, "cotangent": cotangent}


def silu_parts(pre_gate):
    sigmoid_val = jax.nn.sigmoid(pre_gate)
    return pre_gate * sigmoid_val, sigmoid_val * (1.0 + pre_gate * (1.0 - sigmoid_val))


def contract_rows(left_rows, right_rows):
    return lax.dot_general(left_rows, right_rows, (((0,), (0,)), ((), ())), preferred_element_type=jnp.float32)


def contract_cols(left_rows, right_rows):
    return lax.dot_general(left_rows, right_rows, (((1,), (1,)), ((), ())), preferred_element_type=jnp.float32)


def expert_forward(rows_in, gate_full, up_full, down_full):
    pre_gate = jnp.dot(rows_in, gate_full, preferred_element_type=jnp.float32)
    pre_up = jnp.dot(rows_in, up_full, preferred_element_type=jnp.float32)
    activation, derivative = silu_parts(pre_gate)
    hidden = (activation * pre_up).astype(jnp.bfloat16)
    expert_out = jnp.dot(hidden, down_full, preferred_element_type=jnp.float32).astype(jnp.bfloat16)
    return expert_out, (pre_up, activation, derivative, hidden)


def expert_backward(rows_in, scaled, saved, gate_full, up_full, down_full):
    pre_up, activation, derivative, hidden = saved
    hidden_grad = contract_cols(scaled, down_full)
    gate_pre = (hidden_grad * pre_up * derivative).astype(jnp.bfloat16)
    up_pre = (hidden_grad * activation).astype(jnp.bfloat16)
    slot_grad = (contract_cols(gate_pre, gate_full) + contract_cols(up_pre, up_full)).astype(jnp.bfloat16)
    return slot_grad, contract_rows(rows_in, gate_pre), contract_rows(rows_in, up_pre), contract_rows(hidden, scaled)


def slot_table(flat_ids, experts, slot_cap):
    total_pairs = flat_ids.shape[0]
    onehot = (flat_ids[:, None] == jnp.arange(experts, dtype=jnp.int32)[None, :]).astype(jnp.int32)
    before = jnp.cumsum(onehot, axis=0) - onehot
    position = jnp.sum(before * onehot, axis=1)
    slot_of = (flat_ids * slot_cap + position).astype(jnp.int32)
    lookup = jnp.full((experts * slot_cap,), total_pairs, jnp.int32)
    lookup = lookup.at[slot_of].set(jnp.arange(total_pairs, dtype=jnp.int32))
    return lookup, slot_of


def reference(tokens, expert_ids, gate_quant, bucket_ids, bucket_counts, gate_weight, up_weight, down_weight, cotangent):
    experts = gate_weight.shape[0]
    top_count = expert_ids.shape[1]
    group_size = N_EP * TOK_DEV
    slot_cap = N_EP * CAP
    model_width = tokens.shape[1]
    gate_share = gate_quant.astype(jnp.float32) / 1024.0
    token_scale = 64.0 / (64.0 + bucket_counts[bucket_ids].astype(jnp.float32))
    scaled_share = gate_share * token_scale[:, None]
    out_parts = []
    grad_parts = []
    totals = None
    for group_idx in range(N_DP):
        first_row = group_idx * group_size
        group_tokens = tokens[first_row:first_row + group_size]
        group_cot = cotangent[first_row:first_row + group_size]
        flat_ids = expert_ids[first_row:first_row + group_size].reshape(-1)
        gate_flat = gate_share[first_row:first_row + group_size].reshape(-1)
        scaled_flat = scaled_share[first_row:first_row + group_size].reshape(-1)
        lookup, slot_of = slot_table(flat_ids, experts, slot_cap)
        total_pairs = flat_ids.shape[0]

        def per_expert(running, expert_item):
            out_acc, grad_acc = running
            pair_index, gate_full, up_full, down_full = expert_item
            is_live = pair_index < total_pairs
            safe_index = jnp.where(is_live, pair_index, 0).astype(jnp.int32)
            source_row = (safe_index // top_count).astype(jnp.int32)
            rows_in = jnp.where(is_live[:, None], group_tokens[source_row], jnp.zeros((), jnp.bfloat16)).astype(jnp.bfloat16)
            gate_slot = jnp.where(is_live, gate_flat[safe_index], jnp.zeros((), jnp.float32))
            scale_slot = jnp.where(is_live, scaled_flat[safe_index], jnp.zeros((), jnp.float32))
            scaled = (scale_slot[:, None] * group_cot[source_row].astype(jnp.float32)).astype(jnp.bfloat16)
            expert_out, saved = expert_forward(rows_in, gate_full, up_full, down_full)
            slot_grad, grad_gate, grad_up, grad_down = expert_backward(rows_in, scaled, saved, gate_full, up_full, down_full)
            out_acc = out_acc.at[source_row].add(gate_slot[:, None] * expert_out.astype(jnp.float32))
            grad_acc = grad_acc.at[source_row].add(jnp.where(is_live[:, None], slot_grad.astype(jnp.float32), jnp.zeros((), jnp.float32)))
            return (out_acc, grad_acc), (grad_gate.astype(jnp.bfloat16), grad_up.astype(jnp.bfloat16), grad_down.astype(jnp.bfloat16))

        start_acc = (jnp.zeros((group_size, model_width), jnp.float32), jnp.zeros((group_size, model_width), jnp.float32))
        stacked = (lookup.reshape(experts, slot_cap), gate_weight, up_weight, down_weight)
        (out_acc, grad_acc), partials = lax.scan(per_expert, start_acc, stacked)
        out_parts.append(out_acc.astype(jnp.bfloat16))
        grad_parts.append(grad_acc.astype(jnp.bfloat16))
        widened = tuple(part.astype(jnp.float32) for part in partials)
        if totals is None:
            totals = widened
        else:
            totals = tuple(acc + part for acc, part in zip(totals, widened))
    layer_out = jnp.concatenate(out_parts, axis=0)
    token_grad = jnp.concatenate(grad_parts, axis=0)
    return (layer_out, token_grad, totals[0], totals[1], totals[2])
```

```python
import jax
import jax.numpy as jnp
from jax import lax
from jax.experimental import pallas as pl
from jax.experimental.pallas import tpu as pltpu
from jax.sharding import PartitionSpec as P

MESH = pl.DeviceIdType.MESH
BF = jnp.bfloat16
F32 = jnp.float32
NX, NY, NZ, NC = 4, 8, 8, 2
NE = NY * NZ * NC
LANES = 128


def dot(a, b, ca=1, cb=0):
    return lax.dot_general(a, b, (((ca,), (cb,)), ((), ())), preferred_element_type=F32)


def rows(ref, start, size):
    return ref.at[pl.ds(pl.multiple_of(start, 16), size)]


def kernel(
    bucket_ids,
    bucket_counts,
    tokens,
    cotangent,
    expert_ids,
    gate_quant,
    gate_own,
    up_own,
    down_own,
    layer_out,
    token_grad,
    gate_grad,
    up_grad,
    down_grad,
    gate_full,
    up_full,
    down_full,
    send,
    recv,
    back_send,
    back_recv,
    spread,
    rows_in,
    scaled,
    part_gate,
    part_up,
    part_down,
    hop_gate,
    hop_up,
    hop_down,
    fwd_gate,
    fwd_up,
    fwd_down,
    fin_gate,
    fin_up,
    fin_down,
    step_sem,
    ag_send,
    ag_recv,
    rs_send,
    rs_recv,
    out_send,
    out_recv,
    ret_send,
    ret_recv,
):
    x = lax.axis_index("dp")
    e = lax.axis_index("ep")
    y, z, c = e // (NZ * NC), (e // NC) % NZ, e % NC
    tok_rows, top = expert_ids.shape
    width = tokens.shape[1]
    blocks = width // LANES
    slot = 2 * blocks

    def ep(yy, zz, cc):
        return (lax.rem(yy + NY, NY) * NZ + lax.rem(zz + NZ, NZ)) * NC + lax.rem(cc, NC)

    right, left, across = lax.rem(x + 1, NX), lax.rem(x + NX - 1, NX), lax.rem(x + 2, NX)
    y_near = [ep(y + d, z, c) for d in (1, -1)]
    z_near = [ep(y, z + d, c + k) for d in (1, -1) for k in (0, 1)]
    mate = ep(y, z, c + 1)

    barrier = pltpu.get_barrier_semaphore()
    for xx in (right, left):
        pl.semaphore_signal(barrier, inc=1, device_id=(xx, e), device_id_type=MESH)
    for d in (*y_near, *z_near, mate):
        pl.semaphore_signal(barrier, inc=1, device_id=(x, d), device_id_type=MESH)

    lane = lax.broadcasted_iota(jnp.int32, (tok_rows, NE), 1)
    hit = jnp.zeros((tok_rows, NE), F32)
    share = jnp.zeros((tok_rows, NE), F32)
    for k in range(top):
        here = lane == expert_ids[:, k : k + 1]
        hit = hit + jnp.where(here, 1.0, 0.0)
        share = share + jnp.where(here, gate_quant[:, k : k + 1].astype(F32), 0.0)
    share = share / 1024.0
    row = lax.broadcasted_iota(jnp.int32, (tok_rows, NE), 0)
    count = jnp.zeros((tok_rows, NE), jnp.int32)
    for t in range(tok_rows):
        count = jnp.where(row == t, bucket_counts[bucket_ids[t]], count)
    scale = share * (64.0 / (64.0 + count.astype(F32)))
    scale_col = jnp.sum(jnp.transpose(scale), axis=1, keepdims=True)
    pick = hit.astype(BF)
    picked = dot(pick, tokens[...], 0, 0)
    for j in range(blocks):
        spread[pl.ds(j, NE, stride=slot), :] = picked[:, j * LANES : (j + 1) * LANES]
    picked = dot(pick, cotangent[...], 0, 0) * scale_col
    for j in range(blocks):
        spread[pl.ds(blocks + j, NE, stride=slot), :] = picked[:, j * LANES : (j + 1) * LANES]
    send[...] = spread[...].astype(BF)

    pl.semaphore_wait(barrier, 9)

    shards = ((gate_own, gate_full), (up_own, up_full), (down_own, down_full))

    def ag_copy(src, dst, kind, i, xx):
        return pltpu.make_async_remote_copy(
            src, dst, ag_send.at[kind, i], ag_recv.at[kind, i], device_id=(xx, e), device_id_type=MESH
        )

    own_right, own_left = [], []
    for i, (own, full) in enumerate(shards):
        size = own.shape[1]
        target = rows(full, x * size, size)
        own_right.append(ag_copy(own.at[0], target, 0, i, right))
        own_left.append(ag_copy(own.at[0], target, 1, i, left))
        own_right[i].start()
        own_left[i].start()

    for s in range(NY // 2 - 1):
        for d in y_near:
            pl.semaphore_signal(step_sem.at[s], inc=1, device_id=(x, d), device_id_type=MESH)
        pl.semaphore_wait(step_sem.at[s], 2)
    for s in range(NZ // 2):
        n = NY // 2 - 1 + s
        peers = (*z_near, mate) if s == 0 else z_near
        for d in peers:
            pl.semaphore_signal(step_sem.at[n], inc=1, device_id=(x, d), device_id_type=MESH)
        pl.semaphore_wait(step_sem.at[n], len(peers))

    def exchange(src, dst, s_sem, r_sem):
        def one(i, carry):
            d = ep(y + i % NY, z + (i // NY) % NZ, c + i // (NY * NZ))
            pltpu.make_async_remote_copy(
                rows(src, d * slot, slot),
                rows(dst, e * slot, slot),
                s_sem,
                r_sem,
                device_id=(x, d),
                device_id_type=MESH,
            ).start()
            return carry

        lax.fori_loop(1, NE, one, 0)
        at = pl.multiple_of(e * slot, slot)
        dst[pl.ds(at, slot), :] = src[pl.ds(at, slot), :]

    def wait_all(ref, sem):
        part = ref.at[pl.ds(0, (NE - 1) * slot)]
        pltpu.make_async_copy(part, part, sem).wait()

    exchange(send, recv, out_send, out_recv)

    forwards = []
    for i, (own, full) in enumerate(shards):
        size = own.shape[1]
        half = size // 2
        full[pl.ds(pl.multiple_of(x * size, 16), size), :] = own[0]
        own_right[i].wait_recv()
        part = rows(full, left * size, half)
        forwards.append(ag_copy(part, part, 2, i, right))
        forwards[-1].start()
        own_left[i].wait_recv()
        part = rows(full, right * size + half, half)
        forwards.append(ag_copy(part, part, 3, i, left))
        forwards[-1].start()

    wait_all(recv, out_recv)
    spread[...] = recv[...].astype(F32)
    for j in range(blocks):
        at = slice(j * LANES, (j + 1) * LANES)
        rows_in[:, at] = spread[pl.ds(j, NE, stride=slot), :].astype(BF)
        scaled[:, at] = spread[pl.ds(blocks + j, NE, stride=slot), :].astype(BF)
    for f in forwards[:4]:
        f.wait_recv()
    pre_gate = dot(rows_in[...], gate_full[...])
    pre_up = dot(rows_in[...], up_full[...])
    sig = jax.nn.sigmoid(pre_gate)
    act = pre_gate * sig
    hidden = (act * pre_up).astype(BF)

    def rs_copy(src, dst, kind, i, xx):
        return pltpu.make_async_remote_copy(
            src, dst, rs_send.at[kind, i], rs_recv.at[kind, i], device_id=(xx, e), device_id_type=MESH
        )

    def scatter(i, part, hop, fin):
        size = part.shape[0] // NX
        half = size // 2
        copies = [
            rs_copy(rows(part, across * size, half), hop.at[0], 0, i, right),
            rs_copy(rows(part, across * size + half, half), hop.at[1], 1, i, left),
            rs_copy(rows(part, right * size + half, half), fin.at[0, 1], 2, i, right),
            rs_copy(rows(part, left * size, half), fin.at[1, 0], 3, i, left),
        ]
        for k in copies:
            k.start()
        return copies

    def pass_on(i, part, hop, fwd, fin, copies):
        size = part.shape[0] // NX
        half = size // 2
        copies[0].wait_recv()
        mine = part[pl.ds(pl.multiple_of(right * size, 16), half), :]
        fwd[0] = (hop[0].astype(F32) + mine.astype(F32)).astype(BF)
        copies.append(rs_copy(fwd.at[0], fin.at[0, 0], 4, i, right))
        copies[-1].start()
        copies[1].wait_recv()
        mine = part[pl.ds(pl.multiple_of(left * size + half, 16), half), :]
        fwd[1] = (hop[1].astype(F32) + mine.astype(F32)).astype(BF)
        copies.append(rs_copy(fwd.at[1], fin.at[1, 1], 5, i, left))
        copies[-1].start()

    part_down[...] = dot(hidden, scaled[...], 0, 0).astype(BF)
    down_copies = scatter(2, part_down, hop_down, fin_down)

    for f in forwards[4:]:
        f.wait_recv()
    hidden_grad = dot(scaled[...], down_full[...], 1, 1)
    gate_pre = (hidden_grad * pre_up * (sig * (1.0 + pre_gate * (1.0 - sig)))).astype(BF)
    up_pre = (hidden_grad * act).astype(BF)
    part_gate[...] = dot(rows_in[...], gate_pre, 0, 0).astype(BF)
    gate_copies = scatter(0, part_gate, hop_gate, fin_gate)
    part_up[...] = dot(rows_in[...], up_pre, 0, 0).astype(BF)
    up_copies = scatter(1, part_up, hop_up, fin_up)

    expert_out = dot(hidden, down_full[...])
    for j in range(blocks):
        spread[pl.ds(j, NE, stride=slot), :] = expert_out[:, j * LANES : (j + 1) * LANES]
    slot_grad = dot(gate_pre, gate_full[...], 1, 1) + dot(up_pre, up_full[...], 1, 1)
    for j in range(blocks):
        spread[pl.ds(blocks + j, NE, stride=slot), :] = slot_grad[:, j * LANES : (j + 1) * LANES]
    back_send[...] = spread[...].astype(BF)
    exchange(back_send, back_recv, ret_send, ret_recv)

    pass_on(2, part_down, hop_down, fwd_down, fin_down, down_copies)
    pass_on(0, part_gate, hop_gate, fwd_gate, fin_gate, gate_copies)
    pass_on(1, part_up, hop_up, fwd_up, fin_up, up_copies)

    def finish(part, fin, out, copies):
        size = part.shape[0] // NX
        half = size // 2
        for k in copies[2:]:
            k.wait_recv()
        for h in range(2):
            mine = part[pl.ds(pl.multiple_of(x * size + h * half, 16), half), :]
            out[0, h * half : (h + 1) * half, :] = (
                mine.astype(F32) + fin[0, h].astype(F32) + fin[1, h].astype(F32)
            )

    finish(part_down, fin_down, down_grad, down_copies)

    wait_all(back_recv, ret_recv)
    spread[...] = back_recv[...].astype(F32)
    high = share.astype(BF)
    low = (share - high.astype(F32)).astype(BF)
    for j in range(blocks):
        at = slice(j * LANES, (j + 1) * LANES)
        outs = spread[pl.ds(j, NE, stride=slot), :].astype(BF)
        layer_out[:, at] = (dot(high, outs) + dot(low, outs)).astype(BF)
        grads = spread[pl.ds(blocks + j, NE, stride=slot), :].astype(BF)
        token_grad[:, at] = dot(pick, grads).astype(BF)

    finish(part_gate, fin_gate, gate_grad, gate_copies)
    finish(part_up, fin_up, up_grad, up_copies)

    for k in (*own_right, *own_left, *forwards, *down_copies, *gate_copies, *up_copies):
        k.wait_send()
    wait_all(send, out_send)
    wait_all(back_send, ret_send)


def per_device(
    tokens,
    expert_ids,
    gate_quant,
    bucket_ids,
    bucket_counts,
    gate_weight,
    up_weight,
    down_weight,
    cotangent,
):
    width = tokens.shape[1]
    _, share, hidden = gate_weight.shape
    deep = down_weight.shape[1]
    vmem = pl.BlockSpec(memory_space=pltpu.VMEM)
    smem = pl.BlockSpec(memory_space=pltpu.SMEM)
    slots = (NE * 2 * (width // LANES), LANES)

    def pieces(lead):
        return [
            pltpu.VMEM((*lead, share // 2, hidden), BF),
            pltpu.VMEM((*lead, share // 2, hidden), BF),
            pltpu.VMEM((*lead, deep // 2, width), BF),
        ]

    full = [
        pltpu.VMEM((width, hidden), BF),
        pltpu.VMEM((width, hidden), BF),
        pltpu.VMEM((hidden, width), BF),
    ]
    dma = pltpu.SemaphoreType.DMA
    return pl.pallas_call(
        kernel,
        out_shape=[
            jax.ShapeDtypeStruct(tokens.shape, BF),
            jax.ShapeDtypeStruct(tokens.shape, BF),
            jax.ShapeDtypeStruct(gate_weight.shape, F32),
            jax.ShapeDtypeStruct(up_weight.shape, F32),
            jax.ShapeDtypeStruct(down_weight.shape, F32),
        ],
        in_specs=[smem] * 2 + [vmem] * 7,
        out_specs=[vmem] * 5,
        scratch_shapes=[
            *full,
            *[pltpu.VMEM(slots, BF)] * 4,
            pltpu.VMEM(slots, F32),
            *[pltpu.VMEM((NE, width), BF)] * 2,
            *full,
            *pieces((2,)),
            *pieces((2,)),
            *pieces((2, 2)),
            pltpu.SemaphoreType.REGULAR((NY // 2 + NZ // 2 - 1,)),
            dma((4, 3)),
            dma((4, 3)),
            dma((6, 3)),
            dma((6, 3)),
            dma,
            dma,
            dma,
            dma,
        ],
        compiler_params=pltpu.CompilerParams(
            collective_id=0, has_side_effects=True, vmem_limit_bytes=48 * 1024 * 1024
        ),
        name="moe_step",
    )(
        bucket_ids,
        bucket_counts,
        tokens,
        cotangent,
        expert_ids,
        gate_quant,
        gate_weight,
        up_weight,
        down_weight,
    )


def solution(mesh):
    placed = (
        P(("dp", "ep"), None),
        P(("dp", "ep"), None),
        P(("dp", "ep"), None),
        P(("dp", "ep")),
        P(),
        P("ep", "dp", None),
        P("ep", "dp", None),
        P("ep", "dp", None),
        P(("dp", "ep"), None),
    )
    return jax.shard_map(
        per_device,
        mesh=mesh,
        in_specs=placed,
        out_specs=(
            P(("dp", "ep"), None),
            P(("dp", "ep"), None),
            P("ep", "dp", None),
            P("ep", "dp", None),
            P("ep", "dp", None),
        ),
        check_vma=False,
    )
```

```python
import jax
import jax.numpy as jnp
from jax import lax
from jax.experimental import pallas as pl
from jax.experimental.pallas import tpu as pltpu
from jax.sharding import PartitionSpec as P

MESH = pl.DeviceIdType.MESH
BF = jnp.bfloat16
F32 = jnp.float32
NX, NY, NZ, NC = 4, 8, 8, 2
NE = NY * NZ * NC
LANES = 128
NW = 3
GRANT = 67043328


def dot(a, b, ca=1, cb=0):
    return lax.dot_general(a, b, (((ca,), (cb,)), ((), ())), preferred_element_type=F32)


def rows(ref, start, size):
    return ref.at[pl.ds(pl.multiple_of(start, 16), size)]


def kernel(
    ids_hbm,
    counts_hbm,
    tokens_hbm,
    cotangent_hbm,
    experts_hbm,
    quant_hbm,
    gate_own,
    up_own,
    down_own,
    layer_hbm,
    token_hbm,
    gate_hbm,
    up_hbm,
    down_hbm,
    bucket_ids,
    bucket_counts,
    tokens,
    cotangent,
    expert_ids,
    gate_quant,
    gate_full,
    up_full,
    down_full,
    send,
    recv,
    back_send,
    back_recv,
    spread,
    rows_in,
    scaled,
    part_gate,
    part_up,
    part_down,
    hop_gate,
    hop_up,
    hop_down,
    fwd_gate,
    fwd_up,
    fwd_down,
    fin_gate,
    fin_up,
    fin_down,
    layer_out,
    token_grad,
    gate_grad,
    up_grad,
    down_grad,
    in_sem,
    out_sem,
    line_sem,
    ag_send,
    ag_recv,
    rs_send,
    rs_recv,
    out_send,
    out_recv,
    ret_send,
    ret_recv,
):
    x = lax.axis_index("dp")
    e = lax.axis_index("ep")
    y, z, c = e // (NZ * NC), (e // NC) % NZ, e % NC
    tok_rows, top = experts_hbm.shape
    width = tokens_hbm.shape[1]
    blocks = width // LANES
    slot = 2 * blocks

    def ep(yy, zz, cc):
        return (lax.rem(yy + NY, NY) * NZ + lax.rem(zz + NZ, NZ)) * NC + lax.rem(cc, NC)

    right, left, across = lax.rem(x + 1, NX), lax.rem(x + NX - 1, NX), lax.rem(x + 2, NX)
    column = [ep(y + d, z, c) for d in range(1, NY)]
    shifts = [(0, 1)]
    for d in range(1, NZ // 2 + 1):
        shifts += [(dz, dc) for dz in sorted({d, NZ - d}) for dc in range(NC)]

    shards = ((gate_own, gate_full), (up_own, up_full), (down_own, down_full))

    barrier = pltpu.get_barrier_semaphore()
    for xx in (right, left):
        pl.semaphore_signal(barrier, inc=1, device_id=(xx, e), device_id_type=MESH)
    for d in (*column, *[ep(y, z + dz, c + dc) for dz, dc in shifts]):
        pl.semaphore_signal(barrier, inc=1, device_id=(x, d), device_id_type=MESH)

    loads = []
    for i, (own, full) in enumerate(shards):
        size = own.shape[1]
        loads.append(pltpu.make_async_copy(own.at[0], rows(full, x * size, size), in_sem.at[i]))
    small = (
        (experts_hbm, expert_ids),
        (quant_hbm, gate_quant),
        (ids_hbm, bucket_ids),
        (counts_hbm, bucket_counts),
        (tokens_hbm, tokens),
        (cotangent_hbm, cotangent),
    )
    for i, (src, dst) in enumerate(small):
        loads.append(pltpu.make_async_copy(src, dst, in_sem.at[NW + i]))
    for load in loads:
        load.start()
    for load in loads[:NW]:
        load.wait()
    pl.semaphore_wait(barrier, 2 + len(column) + len(shifts))

    def ag_copy(src, dst, kind, i, xx):
        return pltpu.make_async_remote_copy(
            src, dst, ag_send.at[kind, i], ag_recv.at[kind, i], device_id=(xx, e), device_id_type=MESH
        )

    own_right, own_left = [], []
    for i, (own, full) in enumerate(shards):
        size = own.shape[1]
        part = rows(full, x * size, size)
        own_right.append(ag_copy(part, part, 0, i, right))
        own_left.append(ag_copy(part, part, 1, i, left))
        own_right[i].start()
        own_left[i].start()

    for dz, dc in shifts:
        pl.semaphore_signal(
            line_sem.at[dz, dc], inc=1, device_id=(x, ep(y, z + dz, c + dc)), device_id_type=MESH
        )

    for load in loads[NW:]:
        load.wait()
    lane = lax.broadcasted_iota(jnp.int32, (tok_rows, NE), 1)
    hit = jnp.zeros((tok_rows, NE), F32)
    share = jnp.zeros((tok_rows, NE), F32)
    for k in range(top):
        here = lane == expert_ids[:, k : k + 1]
        hit = hit + jnp.where(here, 1.0, 0.0)
        share = share + jnp.where(here, gate_quant[:, k : k + 1].astype(F32), 0.0)
    share = share / 1024.0
    pick = hit.astype(BF)
    picked = dot(pick, tokens[...], 0, 0)
    for j in range(blocks):
        spread[pl.ds(j, NE, stride=slot), :] = picked[:, j * LANES : (j + 1) * LANES]

    row = lax.broadcasted_iota(jnp.int32, (tok_rows, NE), 0)
    count = jnp.zeros((tok_rows, NE), jnp.int32)
    for t in range(tok_rows):
        count = jnp.where(row == t, bucket_counts[bucket_ids[t]], count)
    scale = share * (64.0 / (64.0 + count.astype(F32)))
    scale_col = jnp.sum(jnp.transpose(scale), axis=1, keepdims=True)
    picked = dot(pick, cotangent[...], 0, 0) * scale_col
    for j in range(blocks):
        spread[pl.ds(blocks + j, NE, stride=slot), :] = picked[:, j * LANES : (j + 1) * LANES]

    send[...] = spread[...].astype(BF)

    def exchange(src, dst, s_sem, r_sem, dz, dc):
        base = ep(y, z + dz, c + dc) - y * (NZ * NC)
        for dy in range(NY):
            if dy + dz + dc == 0:
                continue
            d = lax.rem(y + dy, NY) * (NZ * NC) + base
            pltpu.make_async_remote_copy(
                rows(src, d * slot, slot),
                rows(dst, e * slot, slot),
                s_sem,
                r_sem,
                device_id=(x, d),
                device_id_type=MESH,
            ).start()

    def keep(src, dst):
        at = pl.multiple_of(e * slot, slot)
        dst[pl.ds(at, slot), :] = src[pl.ds(at, slot), :]

    def wait_all(ref, sem):
        part = ref.at[pl.ds(0, (NE - 1) * slot)]
        pltpu.make_async_copy(part, part, sem).wait()

    exchange(send, recv, out_send, out_recv, 0, 0)
    for dz, dc in shifts:
        pl.semaphore_wait(line_sem.at[(NZ - dz) % NZ, dc], 1)
        exchange(send, recv, out_send, out_recv, dz, dc)
    keep(send, recv)

    forwards = []
    for i, (own, full) in enumerate(shards):
        size = own.shape[1]
        half = size // 2
        own_right[i].wait_recv()
        part = rows(full, left * size, half)
        forwards.append(ag_copy(part, part, 2, i, right))
        forwards[-1].start()
        own_left[i].wait_recv()
        part = rows(full, right * size + half, half)
        forwards.append(ag_copy(part, part, 3, i, left))
        forwards[-1].start()

    wait_all(recv, out_recv)
    spread[...] = recv[...].astype(F32)
    for j in range(blocks):
        at = slice(j * LANES, (j + 1) * LANES)
        rows_in[:, at] = spread[pl.ds(j, NE, stride=slot), :].astype(BF)
        scaled[:, at] = spread[pl.ds(blocks + j, NE, stride=slot), :].astype(BF)
    for f in forwards[:4]:
        f.wait_recv()
    pre_gate = dot(rows_in[...], gate_full[...])
    pre_up = dot(rows_in[...], up_full[...])
    sig = jax.nn.sigmoid(pre_gate)
    act = pre_gate * sig
    hidden = (act * pre_up).astype(BF)

    def rs_copy(src, dst, kind, i, xx):
        return pltpu.make_async_remote_copy(
            src, dst, rs_send.at[kind, i], rs_recv.at[kind, i], device_id=(xx, e), device_id_type=MESH
        )

    def scatter(i, part, hop, fin):
        size = part.shape[0] // NX
        half = size // 2
        copies = [
            rs_copy(rows(part, across * size, half), hop.at[0], 0, i, right),
            rs_copy(rows(part, across * size + half, half), hop.at[1], 1, i, left),
            rs_copy(rows(part, right * size + half, half), fin.at[0, 1], 2, i, right),
            rs_copy(rows(part, left * size, half), fin.at[1, 0], 3, i, left),
        ]
        for k in copies:
            k.start()
        return copies

    def pass_on(i, part, hop, fwd, fin, copies):
        size = part.shape[0] // NX
        half = size // 2
        copies[0].wait_recv()
        mine = part[pl.ds(pl.multiple_of(right * size, 16), half), :]
        fwd[0] = (hop[0].astype(F32) + mine.astype(F32)).astype(BF)
        copies.append(rs_copy(fwd.at[0], fin.at[0, 0], 4, i, right))
        copies[-1].start()
        copies[1].wait_recv()
        mine = part[pl.ds(pl.multiple_of(left * size + half, 16), half), :]
        fwd[1] = (hop[1].astype(F32) + mine.astype(F32)).astype(BF)
        copies.append(rs_copy(fwd.at[1], fin.at[1, 1], 5, i, left))
        copies[-1].start()

    part_down[...] = dot(hidden, scaled[...], 0, 0).astype(BF)
    down_copies = scatter(2, part_down, hop_down, fin_down)

    for f in forwards[4:]:
        f.wait_recv()
    hidden_grad = dot(scaled[...], down_full[...], 1, 1)
    gate_pre = (hidden_grad * pre_up * (sig * (1.0 + pre_gate * (1.0 - sig)))).astype(BF)
    up_pre = (hidden_grad * act).astype(BF)
    part_gate[...] = dot(rows_in[...], gate_pre, 0, 0).astype(BF)
    gate_copies = scatter(0, part_gate, hop_gate, fin_gate)
    part_up[...] = dot(rows_in[...], up_pre, 0, 0).astype(BF)
    up_copies = scatter(1, part_up, hop_up, fin_up)

    expert_out = dot(hidden, down_full[...])
    for j in range(blocks):
        spread[pl.ds(j, NE, stride=slot), :] = expert_out[:, j * LANES : (j + 1) * LANES]
    slot_grad = dot(gate_pre, gate_full[...], 1, 1) + dot(up_pre, up_full[...], 1, 1)
    for j in range(blocks):
        spread[pl.ds(blocks + j, NE, stride=slot), :] = slot_grad[:, j * LANES : (j + 1) * LANES]
    back_send[...] = spread[...].astype(BF)
    for dz, dc in ((0, 0), *shifts):
        exchange(back_send, back_recv, ret_send, ret_recv, dz, dc)
    keep(back_send, back_recv)

    pass_on(2, part_down, hop_down, fwd_down, fin_down, down_copies)
    pass_on(0, part_gate, hop_gate, fwd_gate, fin_gate, gate_copies)
    pass_on(1, part_up, hop_up, fwd_up, fin_up, up_copies)

    stores = []

    def store(src, dst):
        stores.append(pltpu.make_async_copy(src, dst, out_sem.at[len(stores)]))
        stores[-1].start()

    def finish(part, fin, out, copies):
        size = part.shape[0] // NX
        half = size // 2
        for k in copies[2:]:
            k.wait_recv()
        for h in range(2):
            mine = part[pl.ds(pl.multiple_of(x * size + h * half, 16), half), :]
            out[0, h * half : (h + 1) * half, :] = (
                mine.astype(F32) + fin[0, h].astype(F32) + fin[1, h].astype(F32)
            )

    finish(part_down, fin_down, down_grad, down_copies)
    store(down_grad, down_hbm)

    wait_all(back_recv, ret_recv)
    spread[...] = back_recv[...].astype(F32)
    high = share.astype(BF)
    low = (share - high.astype(F32)).astype(BF)
    for j in range(blocks):
        at = slice(j * LANES, (j + 1) * LANES)
        outs = spread[pl.ds(j, NE, stride=slot), :].astype(BF)
        layer_out[:, at] = (dot(high, outs) + dot(low, outs)).astype(BF)
        grads = spread[pl.ds(blocks + j, NE, stride=slot), :].astype(BF)
        token_grad[:, at] = dot(pick, grads).astype(BF)

    store(layer_out, layer_hbm)
    store(token_grad, token_hbm)
    finish(part_gate, fin_gate, gate_grad, gate_copies)
    store(gate_grad, gate_hbm)
    finish(part_up, fin_up, up_grad, up_copies)
    store(up_grad, up_hbm)

    for k in (*own_right, *own_left, *forwards, *down_copies, *gate_copies, *up_copies):
        k.wait_send()
    wait_all(send, out_send)
    wait_all(back_send, ret_send)
    for k in stores:
        k.wait()


def emit(*refs):
    n = len(refs) // 3
    arrays, outs, held, sem = refs[:n], refs[n : 2 * n], refs[2 * n : 3 * n], refs[3 * n]
    reads = [pltpu.make_async_copy(arrays[i], held[i], sem.at[i]) for i in range(n)]
    writes = [pltpu.make_async_copy(held[i], outs[i], sem.at[n + i]) for i in range(n)]
    for k in reads:
        k.start()
    for i in range(n):
        reads[i].wait()
        writes[i].start()
    for k in writes:
        k.wait()


def per_device(
    tokens,
    expert_ids,
    gate_quant,
    bucket_ids,
    bucket_counts,
    gate_weight,
    up_weight,
    down_weight,
    cotangent,
):
    width = tokens.shape[1]
    _, share, hidden = gate_weight.shape
    deep = down_weight.shape[1]
    hbm = pl.BlockSpec(memory_space=pltpu.HBM)
    slots = (NE * 2 * (width // LANES), LANES)

    def pieces(lead):
        return [
            pltpu.VMEM((*lead, share // 2, hidden), BF),
            pltpu.VMEM((*lead, share // 2, hidden), BF),
            pltpu.VMEM((*lead, deep // 2, width), BF),
        ]

    full = [
        pltpu.VMEM((width, hidden), BF),
        pltpu.VMEM((width, hidden), BF),
        pltpu.VMEM((hidden, width), BF),
    ]
    dma = pltpu.SemaphoreType.DMA
    results = pl.pallas_call(
        kernel,
        out_shape=[
            jax.ShapeDtypeStruct(tokens.shape, BF),
            jax.ShapeDtypeStruct(tokens.shape, BF),
            jax.ShapeDtypeStruct(gate_weight.shape, F32),
            jax.ShapeDtypeStruct(up_weight.shape, F32),
            jax.ShapeDtypeStruct(down_weight.shape, F32),
        ],
        in_specs=[hbm] * 9,
        out_specs=[hbm] * 5,
        scratch_shapes=[
            pltpu.SMEM(bucket_ids.shape, jnp.int32),
            pltpu.SMEM(bucket_counts.shape, jnp.int32),
            pltpu.VMEM(tokens.shape, BF),
            pltpu.VMEM(tokens.shape, BF),
            pltpu.VMEM(expert_ids.shape, jnp.int32),
            pltpu.VMEM(expert_ids.shape, jnp.int32),
            *full,
            *[pltpu.VMEM(slots, BF)] * 4,
            pltpu.VMEM(slots, F32),
            *[pltpu.VMEM((NE, width), BF)] * 2,
            *full,
            *pieces((2,)),
            *pieces((2,)),
            *pieces((2, 2)),
            pltpu.VMEM(tokens.shape, BF),
            pltpu.VMEM(tokens.shape, BF),
            pltpu.VMEM(gate_weight.shape, F32),
            pltpu.VMEM(up_weight.shape, F32),
            pltpu.VMEM(down_weight.shape, F32),
            dma((NW + 6,)),
            dma((5,)),
            pltpu.SemaphoreType.REGULAR((NZ, NC)),
            dma((4, 3)),
            dma((4, 3)),
            dma((6, 3)),
            dma((6, 3)),
            dma,
            dma,
            dma,
            dma,
        ],
        compiler_params=pltpu.CompilerParams(
            collective_id=0, has_side_effects=True, vmem_limit_bytes=GRANT
        ),
        name="moe_step",
    )(
        bucket_ids,
        bucket_counts,
        tokens,
        cotangent,
        expert_ids,
        gate_quant,
        gate_weight,
        up_weight,
        down_weight,
    )
    return pl.pallas_call(
        emit,
        out_shape=[jax.ShapeDtypeStruct(r.shape, r.dtype) for r in results],
        in_specs=[hbm] * len(results),
        out_specs=[hbm] * len(results),
        scratch_shapes=[*[pltpu.VMEM(r.shape, r.dtype) for r in results], dma((2 * len(results),))],
        compiler_params=pltpu.CompilerParams(vmem_limit_bytes=GRANT),
        name="emit",
    )(*results)


def solution(mesh):
    placed = (
        P(("dp", "ep"), None),
        P(("dp", "ep"), None),
        P(("dp", "ep"), None),
        P(("dp", "ep")),
        P(),
        P("ep", "dp", None),
        P("ep", "dp", None),
        P("ep", "dp", None),
        P(("dp", "ep"), None),
    )
    return jax.shard_map(
        per_device,
        mesh=mesh,
        in_specs=placed,
        out_specs=(
            P(("dp", "ep"), None),
            P(("dp", "ep"), None),
            P("ep", "dp", None),
            P("ep", "dp", None),
            P("ep", "dp", None),
        ),
        check_vma=False,
    )
```

```python
import jax
import jax.numpy as jnp
from jax import lax
from jax.experimental import pallas as pl
from jax.experimental.pallas import tpu as pltpu
from jax.sharding import PartitionSpec as P

MESH = pl.DeviceIdType.MESH
BF = jnp.bfloat16
F32 = jnp.float32
NX, NY, NZ, NC = 4, 8, 8, 2
NE = NY * NZ * NC
LANES = 128
NW = 3
GRANT = 67043328 - 1280 * 1024


def dot(a, b, ca=1, cb=0):
    return lax.dot_general(a, b, (((ca,), (cb,)), ((), ())), preferred_element_type=F32)


def rows(ref, start, size):
    return ref.at[pl.ds(pl.multiple_of(start, 16), size)]


def kernel(
    ids_hbm,
    counts_hbm,
    tokens_hbm,
    cotangent_hbm,
    experts_hbm,
    quant_hbm,
    gate_own,
    up_own,
    down_own,
    layer_out,
    token_grad,
    gate_grad,
    up_grad,
    down_grad,
    bucket_ids,
    bucket_counts,
    tokens,
    cotangent,
    expert_ids,
    gate_quant,
    gate_full,
    up_full,
    down_full,
    send,
    recv,
    back_send,
    back_recv,
    spread,
    rows_in,
    scaled,
    part_gate,
    part_up,
    part_down,
    hop_gate,
    hop_up,
    hop_down,
    fwd_gate,
    fwd_up,
    fwd_down,
    fin_gate,
    fin_up,
    fin_down,
    in_sem,
    line_sem,
    ag_send,
    ag_recv,
    rs_send,
    rs_recv,
    out_send,
    out_recv,
    ret_send,
    ret_recv,
):
    x = lax.axis_index("dp")
    e = lax.axis_index("ep")
    y, z, c = e // (NZ * NC), (e // NC) % NZ, e % NC
    tok_rows, top = experts_hbm.shape
    width = tokens_hbm.shape[1]
    blocks = width // LANES
    slot = 2 * blocks

    def ep(yy, zz, cc):
        return (lax.rem(yy + NY, NY) * NZ + lax.rem(zz + NZ, NZ)) * NC + lax.rem(cc, NC)

    right, left, across = lax.rem(x + 1, NX), lax.rem(x + NX - 1, NX), lax.rem(x + 2, NX)
    column = [ep(y + d, z, c) for d in range(1, NY)]
    shifts = [(0, 1)]
    for d in range(1, NZ // 2 + 1):
        shifts += [(dz, dc) for dz in sorted({d, NZ - d}) for dc in range(NC)]

    shards = ((gate_own, gate_full), (up_own, up_full), (down_own, down_full))

    barrier = pltpu.get_barrier_semaphore()
    for xx in (right, left):
        pl.semaphore_signal(barrier, inc=1, device_id=(xx, e), device_id_type=MESH)
    for d in (*column, *[ep(y, z + dz, c + dc) for dz, dc in shifts]):
        pl.semaphore_signal(barrier, inc=1, device_id=(x, d), device_id_type=MESH)

    loads = []
    for i, (own, full) in enumerate(shards):
        size = own.shape[1]
        loads.append(pltpu.make_async_copy(own.at[0], rows(full, x * size, size), in_sem.at[i]))
    small = (
        (experts_hbm, expert_ids),
        (quant_hbm, gate_quant),
        (ids_hbm, bucket_ids),
        (counts_hbm, bucket_counts),
        (tokens_hbm, tokens),
        (cotangent_hbm, cotangent),
    )
    for i, (src, dst) in enumerate(small):
        loads.append(pltpu.make_async_copy(src, dst, in_sem.at[NW + i]))
    for load in loads:
        load.start()
    for load in loads[:NW]:
        load.wait()
    pl.semaphore_wait(barrier, 2 + len(column) + len(shifts))

    def ag_copy(src, dst, kind, i, xx):
        return pltpu.make_async_remote_copy(
            src, dst, ag_send.at[kind, i], ag_recv.at[kind, i], device_id=(xx, e), device_id_type=MESH
        )

    own_right, own_left = [], []
    for i, (own, full) in enumerate(shards):
        size = own.shape[1]
        part = rows(full, x * size, size)
        own_right.append(ag_copy(part, part, 0, i, right))
        own_left.append(ag_copy(part, part, 1, i, left))
        own_right[i].start()
        own_left[i].start()

    for dz, dc in shifts:
        pl.semaphore_signal(
            line_sem.at[dz, dc], inc=1, device_id=(x, ep(y, z + dz, c + dc)), device_id_type=MESH
        )

    for load in loads[NW:]:
        load.wait()
    lane = lax.broadcasted_iota(jnp.int32, (tok_rows, NE), 1)
    hit = jnp.zeros((tok_rows, NE), F32)
    share = jnp.zeros((tok_rows, NE), F32)
    for k in range(top):
        here = lane == expert_ids[:, k : k + 1]
        hit = hit + jnp.where(here, 1.0, 0.0)
        share = share + jnp.where(here, gate_quant[:, k : k + 1].astype(F32), 0.0)
    share = share / 1024.0
    pick = hit.astype(BF)
    picked = dot(pick, tokens[...], 0, 0)
    for j in range(blocks):
        spread[pl.ds(j, NE, stride=slot), :] = picked[:, j * LANES : (j + 1) * LANES]

    row = lax.broadcasted_iota(jnp.int32, (tok_rows, NE), 0)
    count = jnp.zeros((tok_rows, NE), jnp.int32)
    for t in range(tok_rows):
        count = jnp.where(row == t, bucket_counts[bucket_ids[t]], count)
    scale = share * (64.0 / (64.0 + count.astype(F32)))
    scale_col = jnp.sum(jnp.transpose(scale), axis=1, keepdims=True)
    picked = dot(pick, cotangent[...], 0, 0) * scale_col
    for j in range(blocks):
        spread[pl.ds(blocks + j, NE, stride=slot), :] = picked[:, j * LANES : (j + 1) * LANES]

    send[...] = spread[...].astype(BF)

    def exchange(src, dst, s_sem, r_sem, dz, dc):
        base = ep(y, z + dz, c + dc) - y * (NZ * NC)
        for dy in range(NY):
            if dy + dz + dc == 0:
                continue
            d = lax.rem(y + dy, NY) * (NZ * NC) + base
            pltpu.make_async_remote_copy(
                rows(src, d * slot, slot),
                rows(dst, e * slot, slot),
                s_sem,
                r_sem,
                device_id=(x, d),
                device_id_type=MESH,
            ).start()

    def keep(src, dst):
        at = pl.multiple_of(e * slot, slot)
        dst[pl.ds(at, slot), :] = src[pl.ds(at, slot), :]

    def wait_all(ref, sem):
        part = ref.at[pl.ds(0, (NE - 1) * slot)]
        pltpu.make_async_copy(part, part, sem).wait()

    exchange(send, recv, out_send, out_recv, 0, 0)
    for dz, dc in shifts:
        pl.semaphore_wait(line_sem.at[(NZ - dz) % NZ, dc], 1)
        exchange(send, recv, out_send, out_recv, dz, dc)
    keep(send, recv)

    forwards = []
    for i, (own, full) in enumerate(shards):
        size = own.shape[1]
        half = size // 2
        own_right[i].wait_recv()
        part = rows(full, left * size, half)
        forwards.append(ag_copy(part, part, 2, i, right))
        forwards[-1].start()
        own_left[i].wait_recv()
        part = rows(full, right * size + half, half)
        forwards.append(ag_copy(part, part, 3, i, left))
        forwards[-1].start()

    wait_all(recv, out_recv)
    spread[...] = recv[...].astype(F32)
    for j in range(blocks):
        at = slice(j * LANES, (j + 1) * LANES)
        rows_in[:, at] = spread[pl.ds(j, NE, stride=slot), :].astype(BF)
        scaled[:, at] = spread[pl.ds(blocks + j, NE, stride=slot), :].astype(BF)
    for f in forwards[:4]:
        f.wait_recv()
    pre_gate = dot(rows_in[...], gate_full[...])
    pre_up = dot(rows_in[...], up_full[...])
    sig = jax.nn.sigmoid(pre_gate)
    act = pre_gate * sig
    hidden = (act * pre_up).astype(BF)

    def rs_copy(src, dst, kind, i, xx):
        return pltpu.make_async_remote_copy(
            src, dst, rs_send.at[kind, i], rs_recv.at[kind, i], device_id=(xx, e), device_id_type=MESH
        )

    def scatter(i, part, hop, fin):
        size = part.shape[0] // NX
        half = size // 2
        copies = [
            rs_copy(rows(part, across * size, half), hop.at[0], 0, i, right),
            rs_copy(rows(part, across * size + half, half), hop.at[1], 1, i, left),
            rs_copy(rows(part, right * size + half, half), fin.at[0, 1], 2, i, right),
            rs_copy(rows(part, left * size, half), fin.at[1, 0], 3, i, left),
        ]
        for k in copies:
            k.start()
        return copies

    def pass_on(i, part, hop, fwd, fin, copies):
        size = part.shape[0] // NX
        half = size // 2
        copies[0].wait_recv()
        mine = part[pl.ds(pl.multiple_of(right * size, 16), half), :]
        fwd[0] = (hop[0].astype(F32) + mine.astype(F32)).astype(BF)
        copies.append(rs_copy(fwd.at[0], fin.at[0, 0], 4, i, right))
        copies[-1].start()
        copies[1].wait_recv()
        mine = part[pl.ds(pl.multiple_of(left * size + half, 16), half), :]
        fwd[1] = (hop[1].astype(F32) + mine.astype(F32)).astype(BF)
        copies.append(rs_copy(fwd.at[1], fin.at[1, 1], 5, i, left))
        copies[-1].start()

    part_down[...] = dot(hidden, scaled[...], 0, 0).astype(BF)
    down_copies = scatter(2, part_down, hop_down, fin_down)

    for f in forwards[4:]:
        f.wait_recv()
    hidden_grad = dot(scaled[...], down_full[...], 1, 1)
    gate_pre = (hidden_grad * pre_up * (sig * (1.0 + pre_gate * (1.0 - sig)))).astype(BF)
    up_pre = (hidden_grad * act).astype(BF)
    expert_out = dot(hidden, down_full[...])
    for j in range(blocks):
        spread[pl.ds(j, NE, stride=slot), :] = expert_out[:, j * LANES : (j + 1) * LANES]
    slot_grad = dot(gate_pre, gate_full[...], 1, 1) + dot(up_pre, up_full[...], 1, 1)
    for j in range(blocks):
        spread[pl.ds(blocks + j, NE, stride=slot), :] = slot_grad[:, j * LANES : (j + 1) * LANES]
    back_send[...] = spread[...].astype(BF)
    for dz, dc in ((0, 0), *shifts):
        exchange(back_send, back_recv, ret_send, ret_recv, dz, dc)
    keep(back_send, back_recv)

    part_gate[...] = dot(rows_in[...], gate_pre, 0, 0).astype(BF)
    gate_copies = scatter(0, part_gate, hop_gate, fin_gate)
    part_up[...] = dot(rows_in[...], up_pre, 0, 0).astype(BF)
    up_copies = scatter(1, part_up, hop_up, fin_up)

    pass_on(2, part_down, hop_down, fwd_down, fin_down, down_copies)
    pass_on(0, part_gate, hop_gate, fwd_gate, fin_gate, gate_copies)
    pass_on(1, part_up, hop_up, fwd_up, fin_up, up_copies)

    def finish(part, fin, out, copies):
        size = part.shape[0] // NX
        half = size // 2
        for k in copies[2:]:
            k.wait_recv()
        for h in range(2):
            mine = part[pl.ds(pl.multiple_of(x * size + h * half, 16), half), :]
            out[0, h * half : (h + 1) * half, :] = (
                mine.astype(F32) + fin[0, h].astype(F32) + fin[1, h].astype(F32)
            )

    finish(part_down, fin_down, down_grad, down_copies)

    wait_all(back_recv, ret_recv)
    spread[...] = back_recv[...].astype(F32)
    high = share.astype(BF)
    low = (share - high.astype(F32)).astype(BF)
    for j in range(blocks):
        at = slice(j * LANES, (j + 1) * LANES)
        outs = spread[pl.ds(j, NE, stride=slot), :].astype(BF)
        layer_out[:, at] = (dot(high, outs) + dot(low, outs)).astype(BF)
        grads = spread[pl.ds(blocks + j, NE, stride=slot), :].astype(BF)
        token_grad[:, at] = dot(pick, grads).astype(BF)

    finish(part_gate, fin_gate, gate_grad, gate_copies)
    finish(part_up, fin_up, up_grad, up_copies)

    for k in (*own_right, *own_left, *forwards, *down_copies, *gate_copies, *up_copies):
        k.wait_send()
    wait_all(send, out_send)
    wait_all(back_send, ret_send)


def emit(*refs):
    *arrays, sem = refs
    half = len(arrays) // 2
    copies = [pltpu.make_async_copy(arrays[i], arrays[half + i], sem.at[i]) for i in range(half)]
    for k in copies:
        k.start()
    for k in copies:
        k.wait()


def per_device(
    tokens,
    expert_ids,
    gate_quant,
    bucket_ids,
    bucket_counts,
    gate_weight,
    up_weight,
    down_weight,
    cotangent,
):
    width = tokens.shape[1]
    _, share, hidden = gate_weight.shape
    deep = down_weight.shape[1]
    hbm = pl.BlockSpec(memory_space=pltpu.HBM)
    vmem = pl.BlockSpec(memory_space=pltpu.VMEM)
    slots = (NE * 2 * (width // LANES), LANES)

    def pieces(lead):
        return [
            pltpu.VMEM((*lead, share // 2, hidden), BF),
            pltpu.VMEM((*lead, share // 2, hidden), BF),
            pltpu.VMEM((*lead, deep // 2, width), BF),
        ]

    full = [
        pltpu.VMEM((width, hidden), BF),
        pltpu.VMEM((width, hidden), BF),
        pltpu.VMEM((hidden, width), BF),
    ]
    dma = pltpu.SemaphoreType.DMA
    results = pl.pallas_call(
        kernel,
        out_shape=[
            pltpu.VMEM(tokens.shape, BF),
            pltpu.VMEM(tokens.shape, BF),
            pltpu.VMEM(gate_weight.shape, F32),
            pltpu.VMEM(up_weight.shape, F32),
            pltpu.VMEM(down_weight.shape, F32),
        ],
        in_specs=[hbm] * 9,
        out_specs=[vmem] * 5,
        scratch_shapes=[
            pltpu.SMEM(bucket_ids.shape, jnp.int32),
            pltpu.SMEM(bucket_counts.shape, jnp.int32),
            pltpu.VMEM(tokens.shape, BF),
            pltpu.VMEM(tokens.shape, BF),
            pltpu.VMEM(expert_ids.shape, jnp.int32),
            pltpu.VMEM(expert_ids.shape, jnp.int32),
            *full,
            *[pltpu.VMEM(slots, BF)] * 4,
            pltpu.VMEM(slots, F32),
            *[pltpu.VMEM((NE, width), BF)] * 2,
            *full,
            *pieces((2,)),
            *pieces((2,)),
            *pieces((2, 2)),
            dma((NW + 6,)),
            pltpu.SemaphoreType.REGULAR((NZ, NC)),
            dma((4, 3)),
            dma((4, 3)),
            dma((6, 3)),
            dma((6, 3)),
            dma,
            dma,
            dma,
            dma,
        ],
        compiler_params=pltpu.CompilerParams(
            collective_id=0, has_side_effects=True, vmem_limit_bytes=GRANT
        ),
        name="moe_step",
    )(
        bucket_ids,
        bucket_counts,
        tokens,
        cotangent,
        expert_ids,
        gate_quant,
        gate_weight,
        up_weight,
        down_weight,
    )
    return pl.pallas_call(
        emit,
        out_shape=[jax.ShapeDtypeStruct(r.shape, r.dtype) for r in results],
        in_specs=[vmem] * len(results),
        out_specs=[hbm] * len(results),
        scratch_shapes=[dma((len(results),))],
        compiler_params=pltpu.CompilerParams(vmem_limit_bytes=32 * 1024 * 1024),
        name="emit",
    )(*results)


def solution(mesh):
    placed = (
        P(("dp", "ep"), None),
        P(("dp", "ep"), None),
        P(("dp", "ep"), None),
        P(("dp", "ep")),
        P(),
        P("ep", "dp", None),
        P("ep", "dp", None),
        P("ep", "dp", None),
        P(("dp", "ep"), None),
    )
    return jax.shard_map(
        per_device,
        mesh=mesh,
        in_specs=placed,
        out_specs=(
            P(("dp", "ep"), None),
            P(("dp", "ep"), None),
            P("ep", "dp", None),
            P("ep", "dp", None),
            P("ep", "dp", None),
        ),
        check_vma=False,
    )
```

```python
import jax
import jax.numpy as jnp
from jax import lax
from jax.experimental import pallas as pl
from jax.experimental.pallas import tpu as pltpu
from jax.sharding import PartitionSpec as P

MESH = pl.DeviceIdType.MESH
BF = jnp.bfloat16
F32 = jnp.float32
NX, NY, NZ, NC = 4, 8, 8, 2
NE = NY * NZ * NC
LANES = 128
NW = 3
GRANT = 67043328 - 1280 * 1024


def dot(a, b, ca=1, cb=0):
    return lax.dot_general(a, b, (((ca,), (cb,)), ((), ())), preferred_element_type=F32)


def rows(ref, start, size):
    return ref.at[pl.ds(pl.multiple_of(start, 16), size)]


def kernel(
    ids_hbm,
    counts_hbm,
    tokens_hbm,
    cotangent_hbm,
    experts_hbm,
    quant_hbm,
    gate_own,
    up_own,
    down_own,
    layer_out,
    token_grad,
    gate_grad,
    up_grad,
    down_grad,
    bucket_ids,
    bucket_counts,
    tokens,
    cotangent,
    expert_ids,
    gate_quant,
    gate_full,
    up_full,
    down_full,
    send,
    recv,
    back_send,
    back_recv,
    spread,
    rows_in,
    scaled,
    tok_all,
    pre_all,
    part_down,
    hop_down,
    fwd_down,
    fin_down,
    in_sem,
    line_sem,
    ag_send,
    ag_recv,
    tok_send,
    tok_recv,
    pre_send,
    pre_recv,
    rs_send,
    rs_recv,
    out_send,
    out_recv,
    ret_send,
    ret_recv,
):
    x = lax.axis_index("dp")
    e = lax.axis_index("ep")
    y, z, c = e // (NZ * NC), (e // NC) % NZ, e % NC
    tok_rows, top = experts_hbm.shape
    width = tokens_hbm.shape[1]
    blocks = width // LANES
    slot = 2 * blocks

    def ep(yy, zz, cc):
        return (lax.rem(yy + NY, NY) * NZ + lax.rem(zz + NZ, NZ)) * NC + lax.rem(cc, NC)

    right, left, across = lax.rem(x + 1, NX), lax.rem(x + NX - 1, NX), lax.rem(x + 2, NX)
    column = [ep(y + d, z, c) for d in range(1, NY)]
    shifts = [(0, 1)]
    for d in range(1, NZ // 2 + 1):
        shifts += [(dz, dc) for dz in sorted({d, NZ - d}) for dc in range(NC)]

    shards = ((gate_own, gate_full), (up_own, up_full), (down_own, down_full))

    barrier = pltpu.get_barrier_semaphore()
    for xx in (right, left):
        pl.semaphore_signal(barrier, inc=1, device_id=(xx, e), device_id_type=MESH)
    for d in (*column, *[ep(y, z + dz, c + dc) for dz, dc in shifts]):
        pl.semaphore_signal(barrier, inc=1, device_id=(x, d), device_id_type=MESH)

    loads = []
    for i, (own, full) in enumerate(shards):
        size = own.shape[1]
        loads.append(pltpu.make_async_copy(own.at[0], rows(full, x * size, size), in_sem.at[i]))
    small = (
        (experts_hbm, expert_ids),
        (quant_hbm, gate_quant),
        (ids_hbm, bucket_ids),
        (counts_hbm, bucket_counts),
        (tokens_hbm, tokens),
        (cotangent_hbm, cotangent),
    )
    for i, (src, dst) in enumerate(small):
        loads.append(pltpu.make_async_copy(src, dst, in_sem.at[NW + i]))
    for load in loads:
        load.start()
    pl.semaphore_wait(barrier, 2 + len(column) + len(shifts))

    def ag_copy(src, dst, kind, i, xx):
        return pltpu.make_async_remote_copy(
            src, dst, ag_send.at[kind, i], ag_recv.at[kind, i], device_id=(xx, e), device_id_type=MESH
        )

    own_right, own_left = [], []
    for i, (own, full) in enumerate(shards):
        size = own.shape[1]
        part = rows(full, x * size, size)
        own_right.append(ag_copy(own.at[0], part, 0, i, right))
        own_left.append(ag_copy(own.at[0], part, 1, i, left))
        own_right[i].start()
        own_left[i].start()

    for dz, dc in shifts:
        pl.semaphore_signal(
            line_sem.at[dz, dc], inc=1, device_id=(x, ep(y, z + dz, c + dc)), device_id_type=MESH
        )

    for load in loads:
        load.wait()
    lane = lax.broadcasted_iota(jnp.int32, (tok_rows, NE), 1)
    hit = jnp.zeros((tok_rows, NE), F32)
    share = jnp.zeros((tok_rows, NE), F32)
    for k in range(top):
        here = lane == expert_ids[:, k : k + 1]
        hit = hit + jnp.where(here, 1.0, 0.0)
        share = share + jnp.where(here, gate_quant[:, k : k + 1].astype(F32), 0.0)
    share = share / 1024.0
    pick = hit.astype(BF)
    picked = dot(pick, tokens[...], 0, 0)
    for j in range(blocks):
        spread[pl.ds(j, NE, stride=slot), :] = picked[:, j * LANES : (j + 1) * LANES]

    row = lax.broadcasted_iota(jnp.int32, (tok_rows, NE), 0)
    count = jnp.zeros((tok_rows, NE), jnp.int32)
    for t in range(tok_rows):
        count = jnp.where(row == t, bucket_counts[bucket_ids[t]], count)
    scale = share * (64.0 / (64.0 + count.astype(F32)))
    scale_col = jnp.sum(jnp.transpose(scale), axis=1, keepdims=True)
    picked = dot(pick, cotangent[...], 0, 0) * scale_col
    for j in range(blocks):
        spread[pl.ds(blocks + j, NE, stride=slot), :] = picked[:, j * LANES : (j + 1) * LANES]

    send[...] = spread[...].astype(BF)

    def hops(dy, dz):
        return min(dy, NY - dy) + min(dz, NZ - dz)

    def exchange(src, dst, s_sem, r_sem, where):
        for dy, dz, dc in where:
            d = ep(y + dy, z + dz, c + dc)
            pltpu.make_async_remote_copy(
                rows(src, d * slot, slot),
                rows(dst, e * slot, slot),
                s_sem,
                r_sem,
                device_id=(x, d),
                device_id_type=MESH,
            ).start()

    def line(dz, dc):
        there = [(dy, dz, dc) for dy in range(NY) if dy + dz + dc]
        return sorted(there, key=lambda k: -hops(k[0], k[1]))

    def keep(src, dst):
        at = pl.multiple_of(e * slot, slot)
        dst[pl.ds(at, slot), :] = src[pl.ds(at, slot), :]

    def wait_all(ref, sem):
        part = ref.at[pl.ds(0, (NE - 1) * slot)]
        pltpu.make_async_copy(part, part, sem).wait()

    exchange(send, recv, out_send, out_recv, line(0, 0))
    for dz, dc in shifts:
        pl.semaphore_wait(line_sem.at[(NZ - dz) % NZ, dc], 1)
        exchange(send, recv, out_send, out_recv, line(dz, dc))
    keep(send, recv)

    forwards = []
    for i, (own, full) in enumerate(shards):
        size = own.shape[1]
        half = size // 2
        own_right[i].wait_recv()
        part = rows(full, left * size, half)
        forwards.append(ag_copy(part, part, 2, i, right))
        forwards[-1].start()
        own_left[i].wait_recv()
        part = rows(full, right * size + half, half)
        forwards.append(ag_copy(part, part, 3, i, left))
        forwards[-1].start()

    wait_all(recv, out_recv)
    spread[...] = recv[...].astype(F32)
    per = blocks // NX
    for j in range(blocks):
        at = slice(j % per * LANES, (j % per + 1) * LANES)
        rows_in[j // per, :, at] = spread[pl.ds(j, NE, stride=slot), :].astype(BF)

    tok_copies = []
    for i, xx in enumerate((right, left, across)):
        tok_copies.append(
            pltpu.make_async_remote_copy(
                rows_in.at[xx],
                tok_all.at[x],
                tok_send.at[i],
                tok_recv.at[i],
                device_id=(xx, e),
                device_id_type=MESH,
            )
        )
        tok_copies[-1].start()
    for j in range(blocks):
        scaled[:, j * LANES : (j + 1) * LANES] = spread[pl.ds(blocks + j, NE, stride=slot), :].astype(BF)
    for f in forwards[:4]:
        f.wait_recv()
    deep = gate_own.shape[1]
    pre_gate = jnp.zeros((NE, gate_full.shape[1]), F32)
    pre_up = jnp.zeros((NE, gate_full.shape[1]), F32)
    for q in range(NX):
        at = slice(q * deep, (q + 1) * deep)
        pre_gate = pre_gate + dot(rows_in[q], gate_full[at, :])
        pre_up = pre_up + dot(rows_in[q], up_full[at, :])
    sig = jax.nn.sigmoid(pre_gate)
    act = pre_gate * sig
    hidden = (act * pre_up).astype(BF)

    def rs_copy(src, dst, kind, xx):
        return pltpu.make_async_remote_copy(
            src, dst, rs_send.at[kind], rs_recv.at[kind], device_id=(xx, e), device_id_type=MESH
        )

    def scatter(part, hop, fin):
        size = part.shape[0] // NX
        half = size // 2
        copies = [
            rs_copy(rows(part, across * size, half), hop.at[0], 0, right),
            rs_copy(rows(part, across * size + half, half), hop.at[1], 1, left),
            rs_copy(rows(part, right * size + half, half), fin.at[0, 1], 2, right),
            rs_copy(rows(part, left * size, half), fin.at[1, 0], 3, left),
        ]
        for k in copies:
            k.start()
        return copies

    def pass_on(part, hop, fwd, fin, copies):
        size = part.shape[0] // NX
        half = size // 2
        copies[0].wait_recv()
        mine = part[pl.ds(pl.multiple_of(right * size, 16), half), :]
        fwd[0] = (hop[0].astype(F32) + mine.astype(F32)).astype(BF)
        copies.append(rs_copy(fwd.at[0], fin.at[0, 0], 4, right))
        copies[-1].start()
        copies[1].wait_recv()
        mine = part[pl.ds(pl.multiple_of(left * size + half, 16), half), :]
        fwd[1] = (hop[1].astype(F32) + mine.astype(F32)).astype(BF)
        copies.append(rs_copy(fwd.at[1], fin.at[1, 1], 5, left))
        copies[-1].start()

    part_down[...] = dot(hidden, scaled[...], 0, 0).astype(BF)
    down_copies = scatter(part_down, hop_down, fin_down)

    for f in forwards[4:]:
        f.wait_recv()
    hidden_grad = dot(scaled[...], down_full[...], 1, 1)
    gate_pre = (hidden_grad * pre_up * (sig * (1.0 + pre_gate * (1.0 - sig)))).astype(BF)
    up_pre = (hidden_grad * act).astype(BF)
    pre_all[x, 0] = gate_pre
    pre_all[x, 1] = up_pre

    def pre_copy(ref, kind, xx):
        return pltpu.make_async_remote_copy(
            ref, ref, pre_send.at[kind], pre_recv.at[kind], device_id=(xx, e), device_id_type=MESH
        )

    pre_copies = [pre_copy(pre_all.at[x], 0, right), pre_copy(pre_all.at[x], 1, left)]
    for k in pre_copies:
        k.start()

    expert_out = dot(hidden, down_full[...])
    for j in range(blocks):
        spread[pl.ds(j, NE, stride=slot), :] = expert_out[:, j * LANES : (j + 1) * LANES]
    slot_grad = dot(gate_pre, gate_full[...], 1, 1) + dot(up_pre, up_full[...], 1, 1)
    for j in range(blocks):
        spread[pl.ds(blocks + j, NE, stride=slot), :] = slot_grad[:, j * LANES : (j + 1) * LANES]
    back_send[...] = spread[...].astype(BF)
    everyone = [k for dz, dc in ((0, 0), *shifts) for k in line(dz, dc)]
    exchange(back_send, back_recv, ret_send, ret_recv, sorted(everyone, key=lambda k: -hops(k[0], k[1])))
    keep(back_send, back_recv)

    pass_on(part_down, hop_down, fwd_down, fin_down, down_copies)
    for kind, xx, source in ((0, right, left), (1, left, right)):
        pre_copies[kind].wait_recv()
        pre_copies.append(pre_copy(pre_all.at[source, kind], 2 + kind, xx))
        pre_copies[-1].start()

    def finish(part, fin, out, copies):
        size = part.shape[0] // NX
        half = size // 2
        for k in copies[2:]:
            k.wait_recv()
        for h in range(2):
            mine = part[pl.ds(pl.multiple_of(x * size + h * half, 16), half), :]
            out[0, h * half : (h + 1) * half, :] = (
                mine.astype(F32) + fin[0, h].astype(F32) + fin[1, h].astype(F32)
            )

    for k in tok_copies:
        k.wait_recv()
    sum_gate = dot(rows_in[x], gate_pre, 0, 0)
    sum_up = dot(rows_in[x], up_pre, 0, 0)
    for xx in (left, right):
        sum_gate = sum_gate + dot(tok_all[xx], pre_all[xx, 0], 0, 0)
        sum_up = sum_up + dot(tok_all[xx], pre_all[xx, 1], 0, 0)
    finish(part_down, fin_down, down_grad, down_copies)
    for k in pre_copies[2:]:
        k.wait_recv()
    gate_grad[0] = sum_gate + dot(tok_all[across], pre_all[across, 0], 0, 0)
    up_grad[0] = sum_up + dot(tok_all[across], pre_all[across, 1], 0, 0)

    wait_all(back_recv, ret_recv)
    spread[...] = back_recv[...].astype(F32)
    high = share.astype(BF)
    low = (share - high.astype(F32)).astype(BF)
    for j in range(blocks):
        at = slice(j * LANES, (j + 1) * LANES)
        outs = spread[pl.ds(j, NE, stride=slot), :].astype(BF)
        layer_out[:, at] = (dot(high, outs) + dot(low, outs)).astype(BF)
        grads = spread[pl.ds(blocks + j, NE, stride=slot), :].astype(BF)
        token_grad[:, at] = dot(pick, grads).astype(BF)

    for k in (*own_right, *own_left, *forwards, *tok_copies, *pre_copies, *down_copies):
        k.wait_send()
    wait_all(send, out_send)
    wait_all(back_send, ret_send)


def emit(*refs):
    *arrays, sem = refs
    half = len(arrays) // 2
    copies = [pltpu.make_async_copy(arrays[i], arrays[half + i], sem.at[i]) for i in range(half)]
    for k in copies:
        k.start()
    for k in copies:
        k.wait()


def per_device(
    tokens,
    expert_ids,
    gate_quant,
    bucket_ids,
    bucket_counts,
    gate_weight,
    up_weight,
    down_weight,
    cotangent,
):
    width = tokens.shape[1]
    _, share, hidden = gate_weight.shape
    deep = down_weight.shape[1]
    hbm = pl.BlockSpec(memory_space=pltpu.HBM)
    vmem = pl.BlockSpec(memory_space=pltpu.VMEM)
    slots = (NE * 2 * (width // LANES), LANES)

    full = [
        pltpu.VMEM((width, hidden), BF),
        pltpu.VMEM((width, hidden), BF),
        pltpu.VMEM((hidden, width), BF),
    ]
    dma = pltpu.SemaphoreType.DMA
    results = pl.pallas_call(
        kernel,
        out_shape=[
            pltpu.VMEM(tokens.shape, BF),
            pltpu.VMEM(tokens.shape, BF),
            pltpu.VMEM(gate_weight.shape, F32),
            pltpu.VMEM(up_weight.shape, F32),
            pltpu.VMEM(down_weight.shape, F32),
        ],
        in_specs=[hbm] * 9,
        out_specs=[vmem] * 5,
        scratch_shapes=[
            pltpu.SMEM(bucket_ids.shape, jnp.int32),
            pltpu.SMEM(bucket_counts.shape, jnp.int32),
            pltpu.VMEM(tokens.shape, BF),
            pltpu.VMEM(tokens.shape, BF),
            pltpu.VMEM(expert_ids.shape, jnp.int32),
            pltpu.VMEM(expert_ids.shape, jnp.int32),
            *full,
            *[pltpu.VMEM(slots, BF)] * 4,
            pltpu.VMEM(slots, F32),
            pltpu.VMEM((NX, NE, share), BF),
            pltpu.VMEM((NE, width), BF),
            pltpu.VMEM((NX, NE, share), BF),
            pltpu.VMEM((NX, 2, NE, hidden), BF),
            pltpu.VMEM((hidden, width), BF),
            pltpu.VMEM((2, deep // 2, width), BF),
            pltpu.VMEM((2, deep // 2, width), BF),
            pltpu.VMEM((2, 2, deep // 2, width), BF),
            dma((NW + 6,)),
            pltpu.SemaphoreType.REGULAR((NZ, NC)),
            dma((4, 3)),
            dma((4, 3)),
            dma((3,)),
            dma((3,)),
            dma((4,)),
            dma((4,)),
            dma((6,)),
            dma((6,)),
            dma,
            dma,
            dma,
            dma,
        ],
        compiler_params=pltpu.CompilerParams(
            collective_id=0, has_side_effects=True, vmem_limit_bytes=GRANT
        ),
        name="moe_step",
    )(
        bucket_ids,
        bucket_counts,
        tokens,
        cotangent,
        expert_ids,
        gate_quant,
        gate_weight,
        up_weight,
        down_weight,
    )
    return pl.pallas_call(
        emit,
        out_shape=[jax.ShapeDtypeStruct(r.shape, r.dtype) for r in results],
        in_specs=[vmem] * len(results),
        out_specs=[hbm] * len(results),
        scratch_shapes=[dma((len(results),))],
        compiler_params=pltpu.CompilerParams(vmem_limit_bytes=32 * 1024 * 1024),
        name="emit",
    )(*results)


def solution(mesh):
    placed = (
        P(("dp", "ep"), None),
        P(("dp", "ep"), None),
        P(("dp", "ep"), None),
        P(("dp", "ep")),
        P(),
        P("ep", "dp", None),
        P("ep", "dp", None),
        P("ep", "dp", None),
        P(("dp", "ep"), None),
    )
    return jax.shard_map(
        per_device,
        mesh=mesh,
        in_specs=placed,
        out_specs=(
            P(("dp", "ep"), None),
            P(("dp", "ep"), None),
            P("ep", "dp", None),
            P("ep", "dp", None),
            P("ep", "dp", None),
        ),
        check_vma=False,
    )
```

```python
import jax
import jax.numpy as jnp
from jax import lax
from jax.experimental import pallas as pl
from jax.experimental.pallas import tpu as pltpu
from jax.sharding import PartitionSpec as P

MESH = pl.DeviceIdType.MESH
BF = jnp.bfloat16
F32 = jnp.float32
NX, NY, NZ, NC = 4, 8, 8, 2
NE = NY * NZ * NC
LANES = 128
NW = 3
GRANT = 67043328 - 1280 * 1024


def dot(a, b, ca=1, cb=0):
    return lax.dot_general(a, b, (((ca,), (cb,)), ((), ())), preferred_element_type=F32)


def rows(ref, start, size):
    return ref.at[pl.ds(pl.multiple_of(start, 16), size)]


def kernel(
    ids_hbm,
    counts_hbm,
    tokens_hbm,
    cotangent_hbm,
    experts_hbm,
    quant_hbm,
    gate_own,
    up_own,
    down_own,
    layer_out,
    token_grad,
    gate_grad,
    up_grad,
    down_grad,
    bucket_ids,
    bucket_counts,
    tokens,
    cotangent,
    expert_ids,
    gate_quant,
    gate_full,
    up_full,
    down_full,
    send,
    recv,
    outs_send,
    outs_recv,
    grads_send,
    grads_recv,
    spread,
    rows_in,
    scaled,
    tok_src,
    ids_all,
    more_send,
    more_recv,
    spread_more,
    tok_all,
    pre_all,
    part_down,
    hop_down,
    fwd_down,
    fin_down,
    in_sem,
    line_sem,
    ag_send,
    ag_recv,
    src_send,
    src_recv,
    src_own,
    ext_send,
    ext_recv,
    pre_send,
    pre_recv,
    rs_send,
    rs_recv,
    out_send,
    out_recv,
    ret_send,
    ret_recv,
):
    x = lax.axis_index("dp")
    e = lax.axis_index("ep")
    y, z, c = e // (NZ * NC), (e // NC) % NZ, e % NC
    tok_rows, top = experts_hbm.shape
    width = tokens_hbm.shape[1]
    blocks = width // LANES
    slot = 2 * blocks
    per = blocks // NX

    def ep(yy, zz, cc):
        return (lax.rem(yy + NY, NY) * NZ + lax.rem(zz + NZ, NZ)) * NC + lax.rem(cc, NC)

    right, left, across = lax.rem(x + 1, NX), lax.rem(x + NX - 1, NX), lax.rem(x + 2, NX)
    column = [ep(y + d, z, c) for d in range(1, NY)]
    shifts = [(0, 1)]
    for d in range(1, NZ // 2 + 1):
        shifts += [(dz, dc) for dz in sorted({d, NZ - d}) for dc in range(NC)]

    shards = ((gate_own, gate_full), (up_own, up_full), (down_own, down_full))

    loads = []
    for i, (own, full) in enumerate(shards):
        size = own.shape[1]
        loads.append(pltpu.make_async_copy(own.at[0], rows(full, x * size, size), in_sem.at[i]))
    small = (
        (experts_hbm, expert_ids),
        (quant_hbm, gate_quant),
        (ids_hbm, bucket_ids),
        (counts_hbm, bucket_counts),
        (tokens_hbm, tokens),
        (cotangent_hbm, cotangent),
    )
    for i, (src, dst) in enumerate(small):
        loads.append(pltpu.make_async_copy(src, dst, in_sem.at[NW + i]))
    for load in loads:
        load.start()

    barrier = pltpu.get_barrier_semaphore()
    for xx in (right, left, across):
        pl.semaphore_signal(barrier, inc=1, device_id=(xx, e), device_id_type=MESH)
    for d in (*column, *[ep(y, z + dz, c + dc) for dz, dc in shifts]):
        pl.semaphore_signal(barrier, inc=1, device_id=(x, d), device_id_type=MESH)

    for load in loads[:NW]:
        load.wait()
    pl.semaphore_wait(barrier, 3 + len(column) + len(shifts))

    def ag_copy(src, dst, kind, i, xx):
        return pltpu.make_async_remote_copy(
            src, dst, ag_send.at[kind, i], ag_recv.at[kind, i], device_id=(xx, e), device_id_type=MESH
        )

    own_right, own_left = [], []
    for i, (own, full) in enumerate(shards):
        size = own.shape[1]
        part = rows(full, x * size, size)
        own_right.append(ag_copy(part, part, 0, i, right))
        own_left.append(ag_copy(part, part, 1, i, left))
        own_right[i].start()
        own_left[i].start()

    for dz, dc in shifts:
        pl.semaphore_signal(
            line_sem.at[dz, dc], inc=1, device_id=(x, ep(y, z + dz, c + dc)), device_id_type=MESH
        )

    for load in loads[NW:]:
        load.wait()

    deep = gate_own.shape[1]

    def columns(q):
        return tokens.at[:, pl.ds(pl.multiple_of(q * deep, LANES), deep)]

    src_copies = []
    for i, xx in enumerate((right, left, across)):
        for n, (src, dst) in enumerate(((columns(xx), tok_src.at[x]), (expert_ids, ids_all.at[x]))):
            src_copies.append(
                pltpu.make_async_remote_copy(
                    src, dst, src_send.at[i, n], src_recv.at[i, n], device_id=(xx, e), device_id_type=MESH
                )
            )
            src_copies[-1].start()
    src_local = pltpu.make_async_copy(columns(x), tok_src.at[x], src_own)
    src_local.start()
    ids_all[x] = expert_ids[...]
    lane = lax.broadcasted_iota(jnp.int32, (tok_rows, NE), 1)
    hit = jnp.zeros((tok_rows, NE), F32)
    share = jnp.zeros((tok_rows, NE), F32)
    for k in range(top):
        here = lane == expert_ids[:, k : k + 1]
        hit = hit + jnp.where(here, 1.0, 0.0)
        share = share + jnp.where(here, gate_quant[:, k : k + 1].astype(F32), 0.0)
    share = share / 1024.0
    pick = hit.astype(BF)
    picked = dot(pick, tokens[...], 0, 0)
    for j in range(blocks):
        spread[pl.ds(j, NE, stride=slot), :] = picked[:, j * LANES : (j + 1) * LANES]

    row = lax.broadcasted_iota(jnp.int32, (tok_rows, NE), 0)
    count = jnp.zeros((tok_rows, NE), jnp.int32)
    for t in range(tok_rows):
        count = jnp.where(row == t, bucket_counts[bucket_ids[t]], count)
    scale = share * (64.0 / (64.0 + count.astype(F32)))
    scale_col = jnp.sum(jnp.transpose(scale), axis=1, keepdims=True)
    picked = dot(pick, cotangent[...], 0, 0) * scale_col
    for j in range(blocks):
        spread[pl.ds(blocks + j, NE, stride=slot), :] = picked[:, j * LANES : (j + 1) * LANES]

    send[...] = spread[...].astype(BF)

    def hops(dy, dz):
        return min(dy, NY - dy) + min(dz, NZ - dz)

    def exchange(src, dst, s_sem, r_sem, where):
        for dy, dz, dc in where:
            d = ep(y + dy, z + dz, c + dc)
            pltpu.make_async_remote_copy(
                rows(src, d * slot, slot),
                rows(dst, e * slot, slot),
                s_sem,
                r_sem,
                device_id=(x, d),
                device_id_type=MESH,
            ).start()

    def line(dz, dc):
        there = [(dy, dz, dc) for dy in range(NY) if dy + dz + dc]
        return sorted(there, key=lambda k: -hops(k[0], k[1]))

    everyone = [k for dz, dc in ((0, 0), *shifts) for k in line(dz, dc)]
    everyone = sorted(everyone, key=lambda k: -hops(k[0], k[1]))

    def keep(src, dst):
        at = pl.multiple_of(e * slot, slot)
        dst[pl.ds(at, slot), :] = src[pl.ds(at, slot), :]

    def wait_all(ref, sem):
        part = ref.at[pl.ds(0, (NE - 1) * slot)]
        pltpu.make_async_copy(part, part, sem).wait()

    exchange(send, recv, out_send, out_recv, line(0, 0))
    for dz, dc in shifts:
        pl.semaphore_wait(line_sem.at[(NZ - dz) % NZ, dc], 1)
        exchange(send, recv, out_send, out_recv, line(dz, dc))
    keep(send, recv)

    forwards = []
    for i, (own, full) in enumerate(shards):
        size = own.shape[1]
        half = size // 2
        own_right[i].wait_recv()
        part = rows(full, left * size, half)
        forwards.append(ag_copy(part, part, 2, i, right))
        forwards[-1].start()
        own_left[i].wait_recv()
        part = rows(full, right * size + half, half)
        forwards.append(ag_copy(part, part, 3, i, left))
        forwards[-1].start()

    for k in src_copies:
        k.wait_recv()
    src_local.wait()
    for g in range(NX):
        found = jnp.zeros((tok_rows, NE), F32)
        for k in range(top):
            found = found + jnp.where(lane == ids_all[g, :, k : k + 1], 1.0, 0.0)
        picked = dot(found.astype(BF), tok_src[g], 0, 0)
        for j in range(per):
            spread_more[pl.ds(g * per + j, NE, stride=blocks), :] = picked[:, j * LANES : (j + 1) * LANES]
    more_send[...] = spread_more[...].reshape(NE, blocks, LANES).astype(BF)
    for dy, dz, dc in everyone:
        d = ep(y + dy, z + dz, c + dc)
        pltpu.make_async_remote_copy(
            more_send.at[d], more_recv.at[e], ext_send, ext_recv, device_id=(x, d), device_id_type=MESH
        ).start()
    more_recv[e] = more_send[e]

    wait_all(recv, out_recv)
    spread[...] = recv[...].astype(F32)
    for j in range(blocks):
        at = slice(j % per * LANES, (j % per + 1) * LANES)
        rows_in[j // per, :, at] = spread[pl.ds(j, NE, stride=slot), :].astype(BF)

    for j in range(blocks):
        scaled[:, j * LANES : (j + 1) * LANES] = spread[pl.ds(blocks + j, NE, stride=slot), :].astype(BF)
    for f in forwards[:4]:
        f.wait_recv()
    pre_gate = jnp.zeros((NE, gate_full.shape[1]), F32)
    pre_up = jnp.zeros((NE, gate_full.shape[1]), F32)
    for q in range(NX):
        at = slice(q * deep, (q + 1) * deep)
        pre_gate = pre_gate + dot(rows_in[q], gate_full[at, :])
        pre_up = pre_up + dot(rows_in[q], up_full[at, :])
    sig = jax.nn.sigmoid(pre_gate)
    act = pre_gate * sig
    hidden = (act * pre_up).astype(BF)

    def rs_copy(src, dst, kind, xx):
        return pltpu.make_async_remote_copy(
            src, dst, rs_send.at[kind], rs_recv.at[kind], device_id=(xx, e), device_id_type=MESH
        )

    def scatter(part, hop, fin):
        size = part.shape[0] // NX
        half = size // 2
        copies = [
            rs_copy(rows(part, across * size, half), hop.at[0], 0, right),
            rs_copy(rows(part, across * size + half, half), hop.at[1], 1, left),
            rs_copy(rows(part, right * size + half, half), fin.at[0, 1], 2, right),
            rs_copy(rows(part, left * size, half), fin.at[1, 0], 3, left),
        ]
        for k in copies:
            k.start()
        return copies

    def pass_on(part, hop, fwd, fin, copies):
        size = part.shape[0] // NX
        half = size // 2
        copies[0].wait_recv()
        mine = part[pl.ds(pl.multiple_of(right * size, 16), half), :]
        fwd[0] = (hop[0].astype(F32) + mine.astype(F32)).astype(BF)
        copies.append(rs_copy(fwd.at[0], fin.at[0, 0], 4, right))
        copies[-1].start()
        copies[1].wait_recv()
        mine = part[pl.ds(pl.multiple_of(left * size + half, 16), half), :]
        fwd[1] = (hop[1].astype(F32) + mine.astype(F32)).astype(BF)
        copies.append(rs_copy(fwd.at[1], fin.at[1, 1], 5, left))
        copies[-1].start()

    for f in forwards[4:]:
        f.wait_recv()
    hidden_grad = dot(scaled[...], down_full[...], 1, 1)
    gate_pre = (hidden_grad * pre_up * (sig * (1.0 + pre_gate * (1.0 - sig)))).astype(BF)
    up_pre = (hidden_grad * act).astype(BF)
    pre_all[x, 0] = gate_pre
    pre_all[x, 1] = up_pre

    def pre_copy(ref, kind, xx):
        return pltpu.make_async_remote_copy(
            ref, ref, pre_send.at[kind], pre_recv.at[kind], device_id=(xx, e), device_id_type=MESH
        )

    pre_copies = [pre_copy(pre_all.at[x], 0, right), pre_copy(pre_all.at[x], 1, left)]
    def give_back(value, first, src, dst, kind):
        for j in range(blocks):
            spread[pl.ds(first + j, NE, stride=blocks), :] = value[:, j * LANES : (j + 1) * LANES]
        src[...] = spread[first : first + NE * blocks, :].reshape(NE, blocks, LANES).astype(BF)
        for dy, dz, dc in everyone:
            d = ep(y + dy, z + dz, c + dc)
            pltpu.make_async_remote_copy(
                src.at[d],
                dst.at[e],
                ret_send.at[kind],
                ret_recv.at[kind],
                device_id=(x, d),
                device_id_type=MESH,
            ).start()
        dst[e] = src[e]

    def wait_back(ref, sem):
        part = ref.at[pl.ds(0, NE - 1)]
        pltpu.make_async_copy(part, part, sem).wait()

    give_back(dot(hidden, down_full[...]), 0, outs_send, outs_recv, 0)
    for k in pre_copies:
        k.start()

    slot_grad = dot(gate_pre, gate_full[...], 1, 1) + dot(up_pre, up_full[...], 1, 1)
    give_back(slot_grad, NE * blocks, grads_send, grads_recv, 1)

    part_down[...] = dot(hidden, scaled[...], 0, 0).astype(BF)
    down_copies = scatter(part_down, hop_down, fin_down)

    pass_on(part_down, hop_down, fwd_down, fin_down, down_copies)
    for kind, xx, source in ((0, right, left), (1, left, right)):
        pre_copies[kind].wait_recv()
        pre_copies.append(pre_copy(pre_all.at[source, kind], 2 + kind, xx))
        pre_copies[-1].start()

    def finish(part, fin, out, copies):
        size = part.shape[0] // NX
        half = size // 2
        for k in copies[2:]:
            k.wait_recv()
        for h in range(2):
            mine = part[pl.ds(pl.multiple_of(x * size + h * half, 16), half), :]
            out[0, h * half : (h + 1) * half, :] = (
                mine.astype(F32) + fin[0, h].astype(F32) + fin[1, h].astype(F32)
            )

    part = more_recv.at[pl.ds(0, NE - 1)]
    pltpu.make_async_copy(part, part, ext_recv).wait()
    spread_more[...] = more_recv[...].astype(F32).reshape(NE * blocks, LANES)
    for g in range(NX):
        for j in range(per):
            tok_all[g, :, j * LANES : (j + 1) * LANES] = spread_more[
                pl.ds(g * per + j, NE, stride=blocks), :
            ].astype(BF)
    sum_gate = dot(rows_in[x], gate_pre, 0, 0)
    sum_up = dot(rows_in[x], up_pre, 0, 0)
    for xx in (left, right):
        sum_gate = sum_gate + dot(tok_all[xx], pre_all[xx, 0], 0, 0)
        sum_up = sum_up + dot(tok_all[xx], pre_all[xx, 1], 0, 0)
    finish(part_down, fin_down, down_grad, down_copies)
    wait_back(outs_recv, ret_recv.at[0])
    spread[: NE * blocks, :] = outs_recv[...].astype(F32).reshape(NE * blocks, LANES)
    high = share.astype(BF)
    low = (share - high.astype(F32)).astype(BF)
    for j in range(blocks):
        part = spread[pl.ds(j, NE, stride=blocks), :].astype(BF)
        layer_out[:, j * LANES : (j + 1) * LANES] = (dot(high, part) + dot(low, part)).astype(BF)

    for k in pre_copies[2:]:
        k.wait_recv()
    gate_grad[0] = sum_gate + dot(tok_all[across], pre_all[across, 0], 0, 0)
    up_grad[0] = sum_up + dot(tok_all[across], pre_all[across, 1], 0, 0)

    wait_back(grads_recv, ret_recv.at[1])
    spread[NE * blocks :, :] = grads_recv[...].astype(F32).reshape(NE * blocks, LANES)
    for j in range(blocks):
        part = spread[pl.ds(NE * blocks + j, NE, stride=blocks), :].astype(BF)
        token_grad[:, j * LANES : (j + 1) * LANES] = dot(pick, part).astype(BF)

    for k in (*own_right, *own_left, *forwards, *src_copies, *pre_copies, *down_copies):
        k.wait_send()
    wait_all(send, out_send)
    wait_back(outs_send, ret_send.at[0])
    wait_back(grads_send, ret_send.at[1])
    part = more_send.at[pl.ds(0, NE - 1)]
    pltpu.make_async_copy(part, part, ext_send).wait()


def emit(*refs):
    *arrays, sem = refs
    half = len(arrays) // 2
    copies = [pltpu.make_async_copy(arrays[i], arrays[half + i], sem.at[i]) for i in range(half)]
    for k in copies:
        k.start()
    for k in copies:
        k.wait()


def per_device(
    tokens,
    expert_ids,
    gate_quant,
    bucket_ids,
    bucket_counts,
    gate_weight,
    up_weight,
    down_weight,
    cotangent,
):
    width = tokens.shape[1]
    _, share, hidden = gate_weight.shape
    deep = down_weight.shape[1]
    hbm = pl.BlockSpec(memory_space=pltpu.HBM)
    vmem = pl.BlockSpec(memory_space=pltpu.VMEM)
    slots = (NE * 2 * (width // LANES), LANES)

    full = [
        pltpu.VMEM((width, hidden), BF),
        pltpu.VMEM((width, hidden), BF),
        pltpu.VMEM((hidden, width), BF),
    ]
    dma = pltpu.SemaphoreType.DMA
    results = pl.pallas_call(
        kernel,
        out_shape=[
            pltpu.VMEM(tokens.shape, BF),
            pltpu.VMEM(tokens.shape, BF),
            pltpu.VMEM(gate_weight.shape, F32),
            pltpu.VMEM(up_weight.shape, F32),
            pltpu.VMEM(down_weight.shape, F32),
        ],
        in_specs=[hbm] * 9,
        out_specs=[vmem] * 5,
        scratch_shapes=[
            pltpu.SMEM(bucket_ids.shape, jnp.int32),
            pltpu.SMEM(bucket_counts.shape, jnp.int32),
            pltpu.VMEM(tokens.shape, BF),
            pltpu.VMEM(tokens.shape, BF),
            pltpu.VMEM(expert_ids.shape, jnp.int32),
            pltpu.VMEM(expert_ids.shape, jnp.int32),
            *full,
            *[pltpu.VMEM(slots, BF)] * 2,
            *[pltpu.VMEM((NE, width // LANES, LANES), BF)] * 4,
            pltpu.VMEM(slots, F32),
            pltpu.VMEM((NX, NE, share), BF),
            pltpu.VMEM((NE, width), BF),
            pltpu.VMEM((NX, tokens.shape[0], share), BF),
            pltpu.VMEM((NX, *expert_ids.shape), jnp.int32),
            *[pltpu.VMEM((NE, width // LANES, LANES), BF)] * 2,
            pltpu.VMEM((NE * (width // LANES), LANES), F32),
            pltpu.VMEM((NX, NE, share), BF),
            pltpu.VMEM((NX, 2, NE, hidden), BF),
            pltpu.VMEM((hidden, width), BF),
            pltpu.VMEM((2, deep // 2, width), BF),
            pltpu.VMEM((2, deep // 2, width), BF),
            pltpu.VMEM((2, 2, deep // 2, width), BF),
            dma((NW + 6,)),
            pltpu.SemaphoreType.REGULAR((NZ, NC)),
            dma((4, 3)),
            dma((4, 3)),
            dma((3, 2)),
            dma((3, 2)),
            dma,
            dma,
            dma,
            dma((4,)),
            dma((4,)),
            dma((6,)),
            dma((6,)),
            dma,
            dma,
            dma((2,)),
            dma((2,)),
        ],
        compiler_params=pltpu.CompilerParams(
            collective_id=0, has_side_effects=True, vmem_limit_bytes=GRANT
        ),
        name="moe_step",
    )(
        bucket_ids,
        bucket_counts,
        tokens,
        cotangent,
        expert_ids,
        gate_quant,
        gate_weight,
        up_weight,
        down_weight,
    )
    return pl.pallas_call(
        emit,
        out_shape=[jax.ShapeDtypeStruct(r.shape, r.dtype) for r in results],
        in_specs=[vmem] * len(results),
        out_specs=[hbm] * len(results),
        scratch_shapes=[dma((len(results),))],
        compiler_params=pltpu.CompilerParams(vmem_limit_bytes=32 * 1024 * 1024),
        name="emit",
    )(*results)


def solution(mesh):
    placed = (
        P(("dp", "ep"), None),
        P(("dp", "ep"), None),
        P(("dp", "ep"), None),
        P(("dp", "ep")),
        P(),
        P("ep", "dp", None),
        P("ep", "dp", None),
        P("ep", "dp", None),
        P(("dp", "ep"), None),
    )
    return jax.shard_map(
        per_device,
        mesh=mesh,
        in_specs=placed,
        out_specs=(
            P(("dp", "ep"), None),
            P(("dp", "ep"), None),
            P("ep", "dp", None),
            P("ep", "dp", None),
            P("ep", "dp", None),
        ),
        check_vma=False,
    )
```

```python
import jax
import jax.numpy as jnp
from jax import lax
from jax.experimental import pallas as pl
from jax.experimental.pallas import tpu as pltpu
from jax.sharding import PartitionSpec as P

MESH = pl.DeviceIdType.MESH
BF = jnp.bfloat16
F32 = jnp.float32
NX, NY, NZ, NC = 4, 8, 8, 2
NE = NY * NZ * NC
LANES = 128
NW = 3
GRANT = 67043328 - 1280 * 1024


def dot(a, b, ca=1, cb=0):
    return lax.dot_general(a, b, (((ca,), (cb,)), ((), ())), preferred_element_type=F32)


def rows(ref, start, size):
    return ref.at[pl.ds(pl.multiple_of(start, 16), size)]


def kernel(
    ids_hbm,
    counts_hbm,
    tokens_hbm,
    cotangent_hbm,
    experts_hbm,
    quant_hbm,
    gate_own,
    up_own,
    down_own,
    layer_out,
    token_grad,
    gate_grad,
    up_grad,
    down_grad,
    bucket_ids,
    bucket_counts,
    tokens,
    cotangent,
    expert_ids,
    gate_quant,
    gate_full,
    up_full,
    down_full,
    send,
    recv,
    outs_send,
    outs_recv,
    grads_send,
    grads_recv,
    spread,
    rows_in,
    scaled,
    tok_src,
    ids_all,
    more_send,
    more_recv,
    spread_more,
    tok_all,
    pre_all,
    part_down,
    hop_down,
    fwd_down,
    fin_down,
    in_sem,
    line_sem,
    ag_send,
    ag_recv,
    src_send,
    src_recv,
    src_own,
    ext_send,
    ext_recv,
    pre_send,
    pre_recv,
    rs_send,
    rs_recv,
    out_send,
    out_recv,
    ret_send,
    ret_recv,
):
    x = lax.axis_index("dp")
    e = lax.axis_index("ep")
    y, z, c = e // (NZ * NC), (e // NC) % NZ, e % NC
    tok_rows, top = experts_hbm.shape
    width = tokens_hbm.shape[1]
    blocks = width // LANES
    slot = 2 * blocks
    per = blocks // NX

    def ep(yy, zz, cc):
        return (lax.rem(yy + NY, NY) * NZ + lax.rem(zz + NZ, NZ)) * NC + lax.rem(cc, NC)

    right, left, across = lax.rem(x + 1, NX), lax.rem(x + NX - 1, NX), lax.rem(x + 2, NX)
    column = [ep(y + d, z, c) for d in range(1, NY)]
    shifts = [(0, 1)]
    for d in range(1, NZ // 2 + 1):
        shifts += [(dz, dc) for dz in sorted({d, NZ - d}) for dc in range(NC)]

    shards = ((gate_own, gate_full), (up_own, up_full), (down_own, down_full))

    loads = []
    for i, (own, full) in enumerate(shards):
        size = own.shape[1]
        loads.append(pltpu.make_async_copy(own.at[0], rows(full, x * size, size), in_sem.at[i]))
    small = (
        (experts_hbm, expert_ids),
        (quant_hbm, gate_quant),
        (ids_hbm, bucket_ids),
        (counts_hbm, bucket_counts),
        (tokens_hbm, tokens),
        (cotangent_hbm, cotangent),
    )
    for i, (src, dst) in enumerate(small):
        loads.append(pltpu.make_async_copy(src, dst, in_sem.at[NW + i]))
    for load in loads:
        load.start()

    barrier = pltpu.get_barrier_semaphore()
    for xx in (right, left, across):
        pl.semaphore_signal(barrier, inc=1, device_id=(xx, e), device_id_type=MESH)
    for d in (*column, *[ep(y, z + dz, c + dc) for dz, dc in shifts]):
        pl.semaphore_signal(barrier, inc=1, device_id=(x, d), device_id_type=MESH)

    for load in loads[:NW]:
        load.wait()
    pl.semaphore_wait(barrier, 3 + len(column) + len(shifts))

    def ag_copy(src, dst, kind, i, xx):
        return pltpu.make_async_remote_copy(
            src, dst, ag_send.at[kind, i], ag_recv.at[kind, i], device_id=(xx, e), device_id_type=MESH
        )

    own_right, own_left = [], []
    for i, (own, full) in enumerate(shards):
        size = own.shape[1]
        part = rows(full, x * size, size)
        own_right.append(ag_copy(part, part, 0, i, right))
        own_left.append(ag_copy(part, part, 1, i, left))
        own_right[i].start()
        own_left[i].start()

    for dz, dc in shifts:
        pl.semaphore_signal(
            line_sem.at[dz, dc], inc=1, device_id=(x, ep(y, z + dz, c + dc)), device_id_type=MESH
        )

    for load in loads[NW:]:
        load.wait()

    deep = gate_own.shape[1]

    def columns(q):
        return tokens.at[:, pl.ds(pl.multiple_of(q * deep, LANES), deep)]

    src_copies = []
    for i, xx in enumerate((right, left, across)):
        for n, (src, dst) in enumerate(((columns(xx), tok_src.at[x]), (expert_ids, ids_all.at[x]))):
            src_copies.append(
                pltpu.make_async_remote_copy(
                    src, dst, src_send.at[i, n], src_recv.at[i, n], device_id=(xx, e), device_id_type=MESH
                )
            )
            src_copies[-1].start()
    src_local = pltpu.make_async_copy(columns(x), tok_src.at[x], src_own)
    src_local.start()
    ids_all[x] = expert_ids[...]
    lane = lax.broadcasted_iota(jnp.int32, (tok_rows, NE), 1)
    hit = jnp.zeros((tok_rows, NE), F32)
    share = jnp.zeros((tok_rows, NE), F32)
    for k in range(top):
        here = lane == expert_ids[:, k : k + 1]
        hit = hit + jnp.where(here, 1.0, 0.0)
        share = share + jnp.where(here, gate_quant[:, k : k + 1].astype(F32), 0.0)
    share = share / 1024.0
    pick = hit.astype(BF)
    picked = dot(pick, tokens[...], 0, 0)
    for j in range(blocks):
        spread[pl.ds(j, NE, stride=slot), :] = picked[:, j * LANES : (j + 1) * LANES]

    row = lax.broadcasted_iota(jnp.int32, (tok_rows, NE), 0)
    count = jnp.zeros((tok_rows, NE), jnp.int32)
    for t in range(tok_rows):
        count = jnp.where(row == t, bucket_counts[bucket_ids[t]], count)
    scale = share * (64.0 / (64.0 + count.astype(F32)))
    scale_col = jnp.sum(jnp.transpose(scale), axis=1, keepdims=True)
    picked = dot(pick, cotangent[...], 0, 0) * scale_col
    for j in range(blocks):
        spread[pl.ds(blocks + j, NE, stride=slot), :] = picked[:, j * LANES : (j + 1) * LANES]

    send[...] = spread[...].astype(BF)

    def hops(dy, dz):
        return min(dy, NY - dy) + min(dz, NZ - dz)

    def exchange(src, dst, s_sem, r_sem, where):
        for dy, dz, dc in where:
            d = ep(y + dy, z + dz, c + dc)
            pltpu.make_async_remote_copy(
                rows(src, d * slot, slot),
                rows(dst, e * slot, slot),
                s_sem,
                r_sem,
                device_id=(x, d),
                device_id_type=MESH,
            ).start()

    def line(dz, dc):
        there = [(dy, dz, dc) for dy in range(NY) if dy + dz + dc]
        return sorted(there, key=lambda k: -hops(k[0], k[1]))

    everyone = [k for dz, dc in ((0, 0), *shifts) for k in line(dz, dc)]
    everyone = sorted(everyone, key=lambda k: -hops(k[0], k[1]))

    def keep(src, dst):
        at = pl.multiple_of(e * slot, slot)
        dst[pl.ds(at, slot), :] = src[pl.ds(at, slot), :]

    def wait_all(ref, sem):
        part = ref.at[pl.ds(0, (NE - 1) * slot)]
        pltpu.make_async_copy(part, part, sem).wait()

    exchange(send, recv, out_send, out_recv, line(0, 0))
    for dz, dc in shifts:
        pl.semaphore_wait(line_sem.at[(NZ - dz) % NZ, dc], 1)
        exchange(send, recv, out_send, out_recv, line(dz, dc))
    keep(send, recv)

    forwards = []
    for i, (own, full) in enumerate(shards):
        size = own.shape[1]
        half = size // 2
        own_right[i].wait_recv()
        part = rows(full, left * size, half)
        forwards.append(ag_copy(part, part, 2, i, right))
        forwards[-1].start()
        own_left[i].wait_recv()
        part = rows(full, right * size + half, half)
        forwards.append(ag_copy(part, part, 3, i, left))
        forwards[-1].start()

    for k in src_copies:
        k.wait_recv()
    src_local.wait()
    for g in range(NX):
        found = jnp.zeros((tok_rows, NE), F32)
        for k in range(top):
            found = found + jnp.where(lane == ids_all[g, :, k : k + 1], 1.0, 0.0)
        picked = dot(found.astype(BF), tok_src[g], 0, 0)
        for j in range(per):
            spread_more[pl.ds(g * per + j, NE, stride=blocks), :] = picked[:, j * LANES : (j + 1) * LANES]
    more_send[...] = spread_more[...].reshape(NE, blocks, LANES).astype(BF)
    for dy, dz, dc in everyone:
        d = ep(y + dy, z + dz, c + dc)
        pltpu.make_async_remote_copy(
            more_send.at[d], more_recv.at[e], ext_send, ext_recv, device_id=(x, d), device_id_type=MESH
        ).start()
    more_recv[e] = more_send[e]

    wait_all(recv, out_recv)
    spread[...] = recv[...].astype(F32)
    for j in range(blocks):
        at = slice(j % per * LANES, (j % per + 1) * LANES)
        rows_in[j // per, :, at] = spread[pl.ds(j, NE, stride=slot), :].astype(BF)

    for j in range(blocks):
        scaled[:, j * LANES : (j + 1) * LANES] = spread[pl.ds(blocks + j, NE, stride=slot), :].astype(BF)
    for f in forwards[:4]:
        f.wait_recv()
    pre_gate = jnp.zeros((NE, gate_full.shape[1]), F32)
    pre_up = jnp.zeros((NE, gate_full.shape[1]), F32)
    for q in range(NX):
        at = slice(q * deep, (q + 1) * deep)
        pre_gate = pre_gate + dot(rows_in[q], gate_full[at, :])
        pre_up = pre_up + dot(rows_in[q], up_full[at, :])
    sig = jax.nn.sigmoid(pre_gate)
    act = pre_gate * sig
    hidden = (act * pre_up).astype(BF)

    def rs_copy(src, dst, kind, xx):
        return pltpu.make_async_remote_copy(
            src, dst, rs_send.at[kind], rs_recv.at[kind], device_id=(xx, e), device_id_type=MESH
        )

    def scatter(part, hop, fin):
        size = part.shape[0] // NX
        half = size // 2
        copies = [
            rs_copy(rows(part, across * size, half), hop.at[0], 0, right),
            rs_copy(rows(part, across * size + half, half), hop.at[1], 1, left),
            rs_copy(rows(part, right * size + half, half), fin.at[0, 1], 2, right),
            rs_copy(rows(part, left * size, half), fin.at[1, 0], 3, left),
        ]
        for k in copies:
            k.start()
        return copies

    def pass_on(part, hop, fwd, fin, copies):
        size = part.shape[0] // NX
        half = size // 2
        copies[0].wait_recv()
        mine = part[pl.ds(pl.multiple_of(right * size, 16), half), :]
        fwd[0] = (hop[0].astype(F32) + mine.astype(F32)).astype(BF)
        copies.append(rs_copy(fwd.at[0], fin.at[0, 0], 4, right))
        copies[-1].start()
        copies[1].wait_recv()
        mine = part[pl.ds(pl.multiple_of(left * size + half, 16), half), :]
        fwd[1] = (hop[1].astype(F32) + mine.astype(F32)).astype(BF)
        copies.append(rs_copy(fwd.at[1], fin.at[1, 1], 5, left))
        copies[-1].start()

    for f in forwards[4:]:
        f.wait_recv()
    hidden_grad = dot(scaled[...], down_full[...], 1, 1)
    gate_pre = (hidden_grad * pre_up * (sig * (1.0 + pre_gate * (1.0 - sig)))).astype(BF)
    up_pre = (hidden_grad * act).astype(BF)
    pre_all[x, 0] = gate_pre
    pre_all[x, 1] = up_pre

    def pre_copy(ref, kind, xx):
        return pltpu.make_async_remote_copy(
            ref, ref, pre_send.at[kind], pre_recv.at[kind], device_id=(xx, e), device_id_type=MESH
        )

    pre_copies = [pre_copy(pre_all.at[x], 0, right), pre_copy(pre_all.at[x], 1, left)]
    def give_back(value, first, src, dst, kind):
        for j in range(blocks):
            spread[pl.ds(first + j, NE, stride=blocks), :] = value[:, j * LANES : (j + 1) * LANES]
        src[...] = spread[first : first + NE * blocks, :].reshape(NE, blocks, LANES).astype(BF)
        for dy, dz, dc in everyone:
            d = ep(y + dy, z + dz, c + dc)
            pltpu.make_async_remote_copy(
                src.at[d],
                dst.at[e],
                ret_send.at[kind],
                ret_recv.at[kind],
                device_id=(x, d),
                device_id_type=MESH,
            ).start()
        dst[e] = src[e]

    def wait_back(ref, sem):
        part = ref.at[pl.ds(0, NE - 1)]
        pltpu.make_async_copy(part, part, sem).wait()

    give_back(dot(hidden, down_full[...]), 0, outs_send, outs_recv, 0)
    for k in pre_copies:
        k.start()

    slot_grad = dot(gate_pre, gate_full[...], 1, 1) + dot(up_pre, up_full[...], 1, 1)
    give_back(slot_grad, NE * blocks, grads_send, grads_recv, 1)

    part_down[...] = dot(hidden, scaled[...], 0, 0).astype(BF)
    down_copies = scatter(part_down, hop_down, fin_down)

    pass_on(part_down, hop_down, fwd_down, fin_down, down_copies)
    for kind, xx, source in ((0, right, left), (1, left, right)):
        pre_copies[kind].wait_recv()
        pre_copies.append(pre_copy(pre_all.at[source, kind], 2 + kind, xx))
        pre_copies[-1].start()

    def finish(part, fin, out, copies):
        size = part.shape[0] // NX
        half = size // 2
        for k in copies[2:]:
            k.wait_recv()
        for h in range(2):
            mine = part[pl.ds(pl.multiple_of(x * size + h * half, 16), half), :]
            out[0, h * half : (h + 1) * half, :] = (
                mine.astype(F32) + fin[0, h].astype(F32) + fin[1, h].astype(F32)
            )

    part = more_recv.at[pl.ds(0, NE - 1)]
    pltpu.make_async_copy(part, part, ext_recv).wait()
    spread_more[...] = more_recv[...].astype(F32).reshape(NE * blocks, LANES)
    for g in range(NX):
        for j in range(per):
            tok_all[g, :, j * LANES : (j + 1) * LANES] = spread_more[
                pl.ds(g * per + j, NE, stride=blocks), :
            ].astype(BF)
    sum_gate = dot(rows_in[x], gate_pre, 0, 0)
    sum_up = dot(rows_in[x], up_pre, 0, 0)
    for xx in (left, right):
        sum_gate = sum_gate + dot(tok_all[xx], pre_all[xx, 0], 0, 0)
        sum_up = sum_up + dot(tok_all[xx], pre_all[xx, 1], 0, 0)
    finish(part_down, fin_down, down_grad, down_copies)
    for k in pre_copies[2:]:
        k.wait_recv()
    gate_grad[0] = sum_gate + dot(tok_all[across], pre_all[across, 0], 0, 0)
    up_grad[0] = sum_up + dot(tok_all[across], pre_all[across, 1], 0, 0)

    wait_back(outs_recv, ret_recv.at[0])
    spread[: NE * blocks, :] = outs_recv[...].astype(F32).reshape(NE * blocks, LANES)
    high = share.astype(BF)
    low = (share - high.astype(F32)).astype(BF)
    for j in range(blocks):
        part = spread[pl.ds(j, NE, stride=blocks), :].astype(BF)
        layer_out[:, j * LANES : (j + 1) * LANES] = (dot(high, part) + dot(low, part)).astype(BF)

    wait_back(grads_recv, ret_recv.at[1])
    spread[NE * blocks :, :] = grads_recv[...].astype(F32).reshape(NE * blocks, LANES)
    for j in range(blocks):
        part = spread[pl.ds(NE * blocks + j, NE, stride=blocks), :].astype(BF)
        token_grad[:, j * LANES : (j + 1) * LANES] = dot(pick, part).astype(BF)

    for k in (*own_right, *own_left, *forwards, *src_copies, *pre_copies, *down_copies):
        k.wait_send()
    wait_all(send, out_send)
    wait_back(outs_send, ret_send.at[0])
    wait_back(grads_send, ret_send.at[1])
    part = more_send.at[pl.ds(0, NE - 1)]
    pltpu.make_async_copy(part, part, ext_send).wait()


def emit(*refs):
    *arrays, sem = refs
    half = len(arrays) // 2
    copies = [pltpu.make_async_copy(arrays[i], arrays[half + i], sem.at[i]) for i in range(half)]
    for k in copies:
        k.start()
    for k in copies:
        k.wait()


def per_device(
    tokens,
    expert_ids,
    gate_quant,
    bucket_ids,
    bucket_counts,
    gate_weight,
    up_weight,
    down_weight,
    cotangent,
):
    width = tokens.shape[1]
    _, share, hidden = gate_weight.shape
    deep = down_weight.shape[1]
    hbm = pl.BlockSpec(memory_space=pltpu.HBM)
    vmem = pl.BlockSpec(memory_space=pltpu.VMEM)
    slots = (NE * 2 * (width // LANES), LANES)

    full = [
        pltpu.VMEM((width, hidden), BF),
        pltpu.VMEM((width, hidden), BF),
        pltpu.VMEM((hidden, width), BF),
    ]
    dma = pltpu.SemaphoreType.DMA
    results = pl.pallas_call(
        kernel,
        out_shape=[
            pltpu.VMEM(tokens.shape, BF),
            pltpu.VMEM(tokens.shape, BF),
            pltpu.VMEM(gate_weight.shape, F32),
            pltpu.VMEM(up_weight.shape, F32),
            pltpu.VMEM(down_weight.shape, F32),
        ],
        in_specs=[hbm] * 9,
        out_specs=[vmem] * 5,
        scratch_shapes=[
            pltpu.SMEM(bucket_ids.shape, jnp.int32),
            pltpu.SMEM(bucket_counts.shape, jnp.int32),
            pltpu.VMEM(tokens.shape, BF),
            pltpu.VMEM(tokens.shape, BF),
            pltpu.VMEM(expert_ids.shape, jnp.int32),
            pltpu.VMEM(expert_ids.shape, jnp.int32),
            *full,
            *[pltpu.VMEM(slots, BF)] * 2,
            *[pltpu.VMEM((NE, width // LANES, LANES), BF)] * 4,
            pltpu.VMEM(slots, F32),
            pltpu.VMEM((NX, NE, share), BF),
            pltpu.VMEM((NE, width), BF),
            pltpu.VMEM((NX, tokens.shape[0], share), BF),
            pltpu.VMEM((NX, *expert_ids.shape), jnp.int32),
            *[pltpu.VMEM((NE, width // LANES, LANES), BF)] * 2,
            pltpu.VMEM((NE * (width // LANES), LANES), F32),
            pltpu.VMEM((NX, NE, share), BF),
            pltpu.VMEM((NX, 2, NE, hidden), BF),
            pltpu.VMEM((hidden, width), BF),
            pltpu.VMEM((2, deep // 2, width), BF),
            pltpu.VMEM((2, deep // 2, width), BF),
            pltpu.VMEM((2, 2, deep // 2, width), BF),
            dma((NW + 6,)),
            pltpu.SemaphoreType.REGULAR((NZ, NC)),
            dma((4, 3)),
            dma((4, 3)),
            dma((3, 2)),
            dma((3, 2)),
            dma,
            dma,
            dma,
            dma((4,)),
            dma((4,)),
            dma((6,)),
            dma((6,)),
            dma,
            dma,
            dma((2,)),
            dma((2,)),
        ],
        compiler_params=pltpu.CompilerParams(
            collective_id=0, has_side_effects=True, vmem_limit_bytes=GRANT
        ),
        name="moe_step",
    )(
        bucket_ids,
        bucket_counts,
        tokens,
        cotangent,
        expert_ids,
        gate_quant,
        gate_weight,
        up_weight,
        down_weight,
    )
    return pl.pallas_call(
        emit,
        out_shape=[jax.ShapeDtypeStruct(r.shape, r.dtype) for r in results],
        in_specs=[vmem] * len(results),
        out_specs=[hbm] * len(results),
        scratch_shapes=[dma((len(results),))],
        compiler_params=pltpu.CompilerParams(vmem_limit_bytes=32 * 1024 * 1024),
        name="emit",
    )(*results)


def solution(mesh):
    placed = (
        P(("dp", "ep"), None),
        P(("dp", "ep"), None),
        P(("dp", "ep"), None),
        P(("dp", "ep")),
        P(),
        P("ep", "dp", None),
        P("ep", "dp", None),
        P("ep", "dp", None),
        P(("dp", "ep"), None),
    )
    return jax.shard_map(
        per_device,
        mesh=mesh,
        in_specs=placed,
        out_specs=(
            P(("dp", "ep"), None),
            P(("dp", "ep"), None),
            P("ep", "dp", None),
            P("ep", "dp", None),
            P("ep", "dp", None),
        ),
        check_vma=False,
    )
```
